32 devices in a mesh: grp: 8 (over y, x, core), loc: 4 (over z).
Axes of the slice: x: 2, y: 2, z: 4, core: 2. Of those that a mesh axis runs over, the one named last changes fastest.
Arguments:
- element_values: float32 [8, 442368], P(None, ('grp', 'loc')), may hold values from -6 to 6
- local_map: int32 [442368], P(('grp', 'loc')), may hold values from 0 to 10647, as said below
- send_node: int32 [32, 3072], P(('grp', 'loc')), may hold values from 0 to 10647, as said below
- send_count: int32 [32, 12], P(('grp', 'loc')), may hold values from 0 to 256, as said below
- recv_slot: int32 [32, 3072], P(('grp', 'loc')), may hold values from 0 to 511, as said below
Outputs:
- summed: float32 [8, 442368], P(None, ('grp', 'loc'))
The draws below stay inside these ranges and needn't reach their ends.
Inputs may be any that keep to these rules, and one draw needn't show every extreme that they name: `local_map`: each device's block lists the nodes of its elements as points of a grid of 22 x 22 x 22 distinct nodes, elements in some order, the grid points numbered in an arbitrary order of the device's own; every number below 10648 appears in each block. `send_node`: the live slots toward one peer name distinct nodes; slots at or past a pair's count hold arbitrary node numbers. `send_count`: counts are zero toward groups past the ends of grp (no wrap), exactly 256 toward the device itself, and between 64 and 256 toward every other peer. `recv_slot`: the live slots from one sender to one owner name distinct owned nodes.
All inputs are finite; a program needn't handle non-finite values.
Results may differ from the reference program's by a relative error of at most 0.0003.
Values sent between devices are 32-bit elements; how exact they have to be, the bound alone decides.
A program may use at most 64 MiB of HBM per device.

```python
import jax
import jax.numpy as jnp
from jax import lax

FIELDS = 8
NODES = 512
EB = 3
ELEMS_DEV = 27
EDGE = 22
LOCAL = 10648
SLOTS = 256
OWNED = 512
ELEMS = 864
N_GRP = 8
N_LOC = 4
DEVICES = 32


def slot_counts(key):
    device = jnp.arange(DEVICES, dtype=jnp.int32)[:, None]
    peer = jnp.arange(3 * N_LOC, dtype=jnp.int32)[None, :]
    group = device // N_LOC
    place = device % N_LOC
    offset = peer // N_LOC - 1
    target = peer % N_LOC
    inside = (group + offset >= 0) & (group + offset < N_GRP)
    itself = (offset == 0) & (target == place)
    drawn = jax.random.randint(jax.random.fold_in(key, 21), (DEVICES, 3 * N_LOC), SLOTS // 4, SLOTS + 1)
    counted = jnp.where(itself, SLOTS, drawn)
    return jnp.where(inside, counted, 0).astype(jnp.int32)


def draw_send_count(key, part):
    return slot_counts(key)


def draw_send_node(key, part):
    counts = slot_counts(key)
    device_keys = jax.random.split(jax.random.fold_in(key, 12), DEVICES)
    orders = jax.vmap(lambda k: jax.random.permutation(k, LOCAL))(device_keys).astype(jnp.int32)
    starts = jax.random.randint(jax.random.fold_in(key, 16), (DEVICES, 3 * N_LOC), 0, LOCAL)
    spots = ((starts[:, :, None] + jnp.arange(SLOTS, dtype=jnp.int32)[None, None, :]) % LOCAL).reshape(DEVICES, 3 * N_LOC * SLOTS)
    chosen = jnp.take_along_axis(orders, spots.astype(jnp.int32), axis=1)
    filler = jax.random.randint(jax.random.fold_in(key, 13), (DEVICES, 3 * N_LOC * SLOTS), 0, LOCAL)
    live_slot = (jnp.arange(SLOTS)[None, None, :] < counts[:, :, None]).reshape(DEVICES, 3 * N_LOC * SLOTS)
    return jnp.where(live_slot, chosen, filler).astype(jnp.int32)


def draw_recv_slot(key, part):
    starts = jax.random.randint(jax.random.fold_in(key, 14), (DEVICES, 3 * N_LOC), 0, OWNED)
    slots_all = (starts[:, :, None] + jnp.arange(SLOTS, dtype=jnp.int32)[None, None, :]) % OWNED
    return slots_all.reshape(DEVICES, 3 * N_LOC * SLOTS).astype(jnp.int32)


def grid_table():
    element = jnp.arange(ELEMS_DEV, dtype=jnp.int32)[:, None]
    node = jnp.arange(NODES, dtype=jnp.int32)[None, :]
    first = 7 * (element // (EB * EB)) + node // 64
    second = 7 * (element // EB % EB) + node // 8 % 8
    third = 7 * (element % EB) + node % 8
    return ((first * EDGE + second) * EDGE + third).astype(jnp.int32)


def one_map(key):
    order = jax.random.permutation(jax.random.fold_in(key, 1), ELEMS_DEV)
    labels = jax.random.permutation(jax.random.fold_in(key, 2), LOCAL).astype(jnp.int32)
    return labels[grid_table()[order].reshape(-1)]


def draw_local_map(key, part):
    device_keys = jax.random.split(jax.random.fold_in(key, 15), DEVICES)
    return jax.vmap(one_map)(device_keys).reshape(-1).astype(jnp.int32)


def shard_levels(own_key, shape, cuts, least, top_value):
    gain, own = 1.0, jax.random.fold_in(own_key, 6)
    for dim, parts in cuts:
        steps = jnp.exp(jax.random.uniform(jax.random.fold_in(own, dim), (parts,), jnp.float32, least / len(cuts), top_value / len(cuts)))
        gain = gain * jnp.repeat(steps, shape[dim] // parts).reshape([-1 if axis == dim else 1 for axis in range(len(shape))])
    return gain


def bell_draw(rng, shape, width, limit, cuts=(), kind=jnp.bfloat16):
    entries = width * jax.random.normal(rng, shape, jnp.float32)
    if cuts:
        entries = entries * shard_levels(rng, shape, cuts, -0.22, 0.18)
    return jnp.clip(entries, -limit, limit).astype(kind)


def setup_inputs(seed: int = 0) -> dict:
    key_of = jax.random.split(jax.random.key(seed), 6)
    return {
        "element_values": bell_draw(key_of[0], (FIELDS, ELEMS * NODES), 1.0, 6.0, ((1, 32),), jnp.float32),
        "local_map": draw_local_map(jax.random.fold_in(key_of[5], 71), 0),
        "send_node": draw_send_node(jax.random.fold_in(key_of[5], 71), 0),
        "send_count": draw_send_count(jax.random.fold_in(key_of[5], 71), 0),
        "recv_slot": draw_recv_slot(jax.random.fold_in(key_of[5], 71), 0),
    }


def peer_ids(device, recv_slot):
    group = device // N_LOC
    place = device % N_LOC
    offset = jnp.arange(3, dtype=jnp.int32)[:, None, None]
    target_loc = jnp.arange(N_LOC, dtype=jnp.int32)[None, :, None]
    position = jnp.arange(SLOTS, dtype=jnp.int32)[None, None, :]
    owner = (jnp.clip(group + offset - 1, 0, N_GRP - 1) * N_LOC + target_loc).astype(jnp.int32)
    column = ((offset * N_LOC + place) * SLOTS + position).astype(jnp.int32)
    owner_b, column_b = jnp.broadcast_arrays(owner, column)
    slot_of = recv_slot[owner_b, column_b]
    return (owner_b * OWNED + slot_of).reshape(-1).astype(jnp.int32)


def reference(element_values, local_map, send_node, send_count, recv_slot):
    span = ELEMS_DEV * NODES

    def assemble(device):
        start = (device * span).astype(jnp.int32)
        block = lax.dynamic_slice_in_dim(element_values, start, span, 1)
        mapping = lax.dynamic_slice_in_dim(local_map, start, span, 0)
        assembled = jnp.zeros((FIELDS, LOCAL), jnp.float32).at[:, mapping].add(block)
        live_slot = (jnp.arange(SLOTS, dtype=jnp.int32)[None, :] < send_count[device][:, None]).reshape(-1)
        picked = jnp.where(live_slot[None, :], jnp.take(assembled, send_node[device], axis=1), jnp.float32(0.0))
        return assembled, mapping, live_slot, picked

    def add_device(totals, device):
        assembled, mapping, live_slot, picked = assemble(device)
        return totals.at[:, peer_ids(device, recv_slot)].add(picked), None

    devices = jnp.arange(DEVICES, dtype=jnp.int32)
    totals, _ = lax.scan(add_device, jnp.zeros((FIELDS, DEVICES * OWNED), jnp.float32), devices)

    def finish(device):
        assembled, mapping, live_slot, picked = assemble(device)
        back = jnp.take(totals, peer_ids(device, recv_slot), axis=1)
        change = jnp.where(live_slot[None, :], back - picked, jnp.float32(0.0))
        combined = assembled.at[:, send_node[device]].add(change)
        return jnp.take(combined, mapping, axis=1)

    spread = lax.map(finish, devices)
    return spread.transpose(1, 0, 2).reshape(FIELDS, DEVICES * span)
```

```python
import functools

import jax
import jax.numpy as jnp
from jax import lax
from jax.experimental import pallas as pl
from jax.experimental.pallas import tpu as pltpu
from jax.sharding import PartitionSpec as P

MESH = pl.DeviceIdType.MESH
F32, BF16, I32 = jnp.float32, jnp.bfloat16, jnp.int32
SIDE = 8
NODES = SIDE**3
ROWS = NODES // 128
PAIR = 256
BATCH = 32


def blocks_along(span):
    edge = round((span // NODES) ** (1 / 3))
    assert edge**3 * NODES == span and 1 < edge <= 3
    return edge


def iota(shape, axis):
    return lax.broadcasted_iota(I32, shape, axis)


def halves(x):
    high = x.astype(BF16)
    low = (x - high.astype(F32)).astype(BF16)
    return jnp.concatenate([high, low], axis=0)


def add_rows(index_ref, value_ref, table_ref):
    def step(b, carry):
        base = pl.multiple_of(b * BATCH, BATCH)
        nodes = [index_ref[base + k] for k in range(BATCH)]
        held = [table_ref[pl.ds(n, 1), :] for n in nodes]
        sums = [held[k] + value_ref[pl.ds(base + k, 1), :] for k in range(BATCH)]
        for k in range(BATCH):
            table_ref[pl.ds(nodes[k], 1), :] = sums[k]
        return carry

    lax.fori_loop(0, index_ref.shape[0] // BATCH, step, 0)


def take_rows(index_ref, table_ref, out_ref):
    def step(b, carry):
        base = pl.multiple_of(b * BATCH, BATCH)
        rows = [table_ref[pl.ds(index_ref[base + k], 1), :] for k in range(BATCH)]
        for k in range(BATCH):
            out_ref[pl.ds(base + k, 1), :] = rows[k]
        return carry

    lax.fori_loop(0, index_ref.shape[0] // BATCH, step, 0)


def to_rows(flat_ref, rows_ref):
    def step(t, carry):
        base = pl.multiple_of(t * 128, 128)
        block = flat_ref[:, pl.ds(base, 128)]
        wide = jnp.concatenate([block] * (128 // block.shape[0]), axis=0)
        rows_ref[pl.ds(base, 128), :] = wide.T
        return carry

    lax.fori_loop(0, flat_ref.shape[1] // 128, step, 0)


def from_rows(rows_ref, flat_ref, put):
    def step(t, carry):
        base = pl.multiple_of(t * 128, 128)
        put(base, rows_ref[pl.ds(base, 128), :].T[: flat_ref.shape[0]])
        return carry

    lax.fori_loop(0, flat_ref.shape[1] // 128, step, 0)


def general_table(map_hbm, value_ref, map_smem, rows_ref, table_ref):
    pltpu.sync_copy(map_hbm, map_smem)
    chunk = 96

    def clear(b, carry):
        base = pl.multiple_of(b * chunk, chunk)
        table_ref[pl.ds(base, chunk), :] = jnp.zeros((chunk, 128), F32)
        return carry

    lax.fori_loop(0, table_ref.shape[0] // chunk, clear, 0)
    to_rows(value_ref, rows_ref)
    add_rows(map_smem, rows_ref, table_ref)


def sweep(ref, edge):
    lane = iota((ref.shape[0], 128), 1)
    zero = jnp.zeros((ref.shape[0], 128), F32)

    def at(px, py, pz, row):
        return pl.ds((((px * edge + py) * edge + pz) * ROWS + row) * 128, 128)

    def line(spots_of, first, last, shift):
        held = [ref[:, s] for s in spots_of]
        for i, s in enumerate(spots_of):
            total = held[i]
            if i + 1 < edge:
                total = total + jnp.where(last, pltpu.roll(held[i + 1], shift, 1), zero)
            if i > 0:
                total = total + jnp.where(first, pltpu.roll(held[i - 1], 128 - shift, 1), zero)
            ref[:, s] = total

    for py in range(edge):
        for pz in range(edge):
            for px in range(edge - 1):
                a, b = at(px, py, pz, ROWS - 1), at(px + 1, py, pz, 0)
                upper, lower = ref[:, a], ref[:, b]
                ref[:, a] = upper + jnp.where(lane >= 64, pltpu.roll(lower, 64, 1), zero)
                ref[:, b] = lower + jnp.where(lane < 64, pltpu.roll(upper, 64, 1), zero)
    y, z = (lane // SIDE) % SIDE, lane % SIDE
    for px in range(edge):
        for pz in range(edge):
            for row in range(ROWS):
                line([at(px, py, pz, row) for py in range(edge)], y == 0, y == SIDE - 1, SIDE * (SIDE - 1))
    for px in range(edge):
        for py in range(edge):
            for row in range(ROWS):
                line([at(px, py, pz, row) for pz in range(edge)], z == 0, z == SIDE - 1, SIDE - 1)


def find_places(lab_ref, edge):
    count = edge**3
    near, mid, far = (lab_ref[pl.ds(k, 32, stride=ROWS), :].astype(F32) for k in (0, 1, ROWS - 1))
    near_t, mid_t, far_t = near.T, mid.T, far.T
    real = (iota((32, 32), 0) < count) & (iota((32, 32), 1) < count)
    sides = (
        (near, near_t, 27, far, far_t, 91),
        (mid, mid_t, 67, mid, mid_t, 123),
        (mid, mid_t, 88, mid, mid_t, 95),
    )
    place = jnp.zeros((32, 1), F32)
    for low, low_t, i, high, high_t, j in sides:
        before = jnp.where(real & (low[:, i : i + 1] == high_t[j : j + 1, :]), 1.0, 0.0)
        before_t = jnp.where(real & (high[:, j : j + 1] == low_t[i : i + 1, :]), 1.0, 0.0)
        steps = jnp.zeros((1, 32), F32)
        if edge > 2:
            steps = jnp.sum(before_t, axis=0, keepdims=True)
        place = place * edge + jnp.sum(before * (1.0 + steps), axis=1, keepdims=True)
    hit = (iota((32, 32), 0) < count) & (place == iota((32, 32), 1).astype(F32))
    who = jnp.sum(jnp.where(hit, iota((32, 32), 0).astype(F32), 0.0), axis=0, keepdims=True)
    times = jnp.sum(jnp.where(hit, 1.0, 0.0), axis=0, keepdims=True)
    wrong = jnp.where((iota((1, 32), 1) < count) & (times != 1.0), 1, 0)
    return jnp.clip(who.astype(I32), 0, count - 1), wrong


def count_mismatches(grid_ref, edge):
    total = jnp.zeros((1, 128), I32)

    def compare(step, low_row, high_row, low_lane, shift, axis):
        length = edge**3 * ROWS - step + (high_row - low_row if axis == 0 else 0)
        rows = edge**3 * ROWS - step * ROWS
        return length, rows

    strides = (edge * edge, edge, 1)
    lane = iota((1, 128), 1)
    y, z = (lane // SIDE) % SIDE, lane % SIDE
    for axis, stride in enumerate(strides):
        rows = (edge**3 - stride) * ROWS
        gap = stride * ROWS
        low = grid_ref[0:rows, :]
        high = grid_ref[gap : gap + rows, :]
        element = iota((rows, 1), 0) // ROWS
        inner = (element // stride) % edge < edge - 1
        if axis == 0:
            low = grid_ref[0 : rows, :]
            high = grid_ref[gap - (ROWS - 1) : gap - (ROWS - 1) + rows, :]
            where = inner & (iota((rows, 1), 0) % ROWS == ROWS - 1) & (lane < 64)
            shift = 64
        elif axis == 1:
            where, shift = inner & (y == 0), 128 - SIDE * (SIDE - 1)
            shift = 128 - SIDE * (SIDE - 1)
        else:
            where, shift = inner & (z == 0), 128 - (SIDE - 1)
        differ = where & (pltpu.roll(low, shift, 1) != high)
        total = total + jnp.sum(jnp.where(differ, 1, 0), axis=0, keepdims=True)
    return total


def assemble_kernel(
    edge, slot_count, value_ref, map_ref, node_ref, count_ref, map_hbm, node_hbm,
    picked_ref, grid_ref, spot_ref, meta_ref,
    lab_ref, order_ref, a_ref, b_ref, u_ref, map_smem, node_smem, rows_ref, table_ref,
):
    count = edge**3
    lines = map_ref.shape[0]
    slots_all = picked_ref.shape[1]
    slot_rows = node_ref.shape[0]
    local = ((SIDE - 1) * edge + 1) ** 3
    tall = (local + 127) // 128
    tall16 = a_ref.shape[0] // 2

    lab_ref[0:lines, :] = map_ref[...]
    lab_ref[lines:, :] = jnp.zeros((lab_ref.shape[0] - lines, 128), I32)
    who, wrong = find_places(lab_ref, edge)
    for s in range(count):
        e = who[0, s]
        meta_ref[s] = e
        grid_ref[:, s * NODES : (s + 1) * NODES] = value_ref[:, pl.ds(pl.multiple_of(e * NODES, NODES), NODES)]
        for r in range(ROWS):
            order_ref[s * ROWS + r : s * ROWS + r + 1, :] = lab_ref[pl.ds(e * ROWS + r, 1), :]

    lane = iota((1, 128), 1)
    first = (lane >= 64, (lane // SIDE) % SIDE > 0, lane % SIDE > 0)
    high_of = iota((tall16, 128), 0).astype(BF16)
    low_of = iota((128, 128), 0).astype(BF16)
    zero = jnp.bfloat16(0)
    for r in range(lines):
        s = r // ROWS
        place = (s // (edge * edge), (s // edge) % edge, s % edge)
        label = order_ref[r : r + 1, :]
        for axis in range(3):
            if place[axis] > 0 and (axis > 0 or r % ROWS == 0):
                label = jnp.where(first[axis], label, -1)
        high = jnp.broadcast_to((label >> 7).astype(BF16), (tall16, 128))
        low = jnp.broadcast_to((label & 127).astype(BF16), (128, 128))
        col = slice(r * 128, (r + 1) * 128)
        within = jnp.broadcast_to((lane + (r % 2) * 128).astype(BF16), (tall16, 128))
        hit = high == high_of
        a_ref[0:tall16, col] = jnp.where(hit, jnp.bfloat16(r // 2), zero)
        a_ref[tall16:, col] = jnp.where(hit, within, zero)
        b_ref[:, col] = jnp.where(low == low_of, jnp.bfloat16(1), zero)
    found = lax.dot_general(a_ref[...], b_ref[...], (((1,), (1,)), ((), ())), preferred_element_type=F32)
    where_is = found[0:tall16] * PAIR + found[tall16:]

    sweep(grid_ref, edge)
    for r in range(lines // 2):
        u_ref[r * 16 : (r + 1) * 16, :] = halves(grid_ref[:, r * PAIR : (r + 1) * PAIR])

    node = node_ref[...]
    high, low = node >> 7, node & 127
    spot = jnp.zeros((slot_rows, 128), F32)
    for h in range(tall):
        row = jnp.broadcast_to(where_is[h : h + 1, :], (slot_rows, 128))
        spot = jnp.where(high == h, jnp.take_along_axis(row, low, axis=1), spot)
    per = slot_count // 128
    row_of = iota((slot_rows, 128), 0)
    limit = jnp.zeros((slot_rows, 128), I32)
    for p in range(slot_rows // per):
        limit = jnp.where(row_of // per == p, count_ref[p], limit)
    live = (row_of % per) * 128 + iota((slot_rows, 128), 1) < limit
    spot_ref[...] = jnp.where(live, spot.astype(I32), -PAIR)

    within_of = iota((PAIR, PAIR), 0).astype(BF16)

    def pick(n, carry):
        spots = jnp.concatenate([spot_ref[pl.ds(2 * n, 1), :], spot_ref[pl.ds(2 * n + 1, 1), :]], axis=1)
        low = jnp.broadcast_to((spots & (PAIR - 1)).astype(BF16), (PAIR, PAIR))
        onehot = jnp.where(low == within_of, jnp.bfloat16(1), zero)
        both = jnp.dot(u_ref[...], onehot, preferred_element_type=F32)
        which = jnp.broadcast_to(spots >> 8, (8, PAIR))
        top = jnp.zeros((8, PAIR), F32)
        low_part = jnp.zeros((8, PAIR), F32)
        for r in range(lines // 2):
            mine = which == r
            top = jnp.where(mine, both[r * 16 : r * 16 + 8], top)
            low_part = jnp.where(mine, both[r * 16 + 8 : r * 16 + 16], low_part)
        picked_ref[:, pl.ds(pl.multiple_of(n * PAIR, PAIR), PAIR)] = top + low_part
        return carry

    lax.fori_loop(0, slots_all // PAIR, pick, 0)

    bad = jnp.sum(count_mismatches(order_ref, edge)) + jnp.sum(wrong)
    meta_ref[31] = bad

    @pl.when(bad > 0)
    def _():
        general_table(map_hbm, value_ref, map_smem, rows_ref, table_ref)
        pltpu.sync_copy(node_hbm, node_smem)
        take_rows(node_smem, table_ref, rows_ref)

        def put(base, block):
            p = base // slot_count
            keep = base - p * slot_count + iota((8, 128), 1) < count_ref[p]
            picked_ref[:, pl.ds(base, 128)] = jnp.where(keep, block, 0.0)

        from_rows(rows_ref, picked_ref, put)


def finish_kernel(
    edge, slot_count, change_ref, spot_ref, grid_ref, meta_ref, count_ref, value_hbm, map_hbm, node_hbm,
    out_ref,
    delta_ref, a_ref, b_ref, map_smem, node_smem, rows_ref, table_ref,
):
    count = edge**3
    slots_all = change_ref.shape[1]
    blocks = delta_ref.shape[1] // PAIR
    zero = jnp.bfloat16(0)
    within_of = iota((PAIR, 128), 0).astype(BF16)
    for q in range(slots_all // 128):
        col = slice(q * 128, (q + 1) * 128)
        both = halves(change_ref[:, col])
        spots = spot_ref[q : q + 1, :]
        low = jnp.broadcast_to((spots & (PAIR - 1)).astype(BF16), (PAIR, 128))
        b_ref[:, col] = jnp.where(low == within_of, jnp.bfloat16(1), zero)
        which = jnp.broadcast_to((spots >> 8).astype(BF16), (16, 128))
        for r in range(blocks):
            a_ref[r * 16 : (r + 1) * 16, col] = jnp.where(which == jnp.bfloat16(r), both, zero)
    spread = lax.dot_general(a_ref[...], b_ref[...], (((1,), (1,)), ((), ())), preferred_element_type=F32)
    for r in range(blocks):
        delta_ref[:, r * PAIR : (r + 1) * PAIR] = spread[r * 16 : r * 16 + 8] + spread[r * 16 + 8 : r * 16 + 16]
    sweep(delta_ref, edge)
    for s in range(count):
        col = slice(s * NODES, (s + 1) * NODES)
        spot = pl.ds(pl.multiple_of(meta_ref[s] * NODES, NODES), NODES)
        out_ref[:, spot] = grid_ref[:, col] + delta_ref[:, col]

    @pl.when(meta_ref[31] > 0)
    def _():
        pltpu.sync_copy(value_hbm, delta_ref)
        general_table(map_hbm, delta_ref, map_smem, rows_ref, table_ref)
        pltpu.sync_copy(node_hbm, node_smem)
        to_rows(change_ref, rows_ref)
        spare = table_ref.shape[0] - 1

        def bury(i, carry):
            p = i // slot_count
            node_smem[i] = jnp.where(i - p * slot_count < count_ref[p], node_smem[i], spare)
            return carry

        lax.fori_loop(0, slots_all, bury, 0)
        add_rows(node_smem, rows_ref, table_ref)
        take_rows(map_smem, table_ref, rows_ref)

        def put(base, block):
            out_ref[:, pl.ds(base, 128)] = block

        from_rows(rows_ref, out_ref, put)


def exchange_kernel(
    groups, places, picked_ref, owned_ref, change_ref,
    inbox, reply, back, a_ref, b_ref, send_out, recv_out, send_back, recv_back,
):
    fields, slots_all = picked_ref.shape
    size = slots_all // (3 * places)
    heads = a_ref.shape[0] // 16
    g, l = lax.axis_index("grp"), lax.axis_index("loc")
    reach = [(g + k - 1 >= 0) & (g + k - 1 < groups) for k in range(3)]
    heard = [(g - k + 1 >= 0) & (g - k + 1 < groups) for k in range(3)]
    peers = [(k, d) for d in range(places) for k in range(3) if (k, d) != (1, 0)]

    def part(k, place):
        return pl.ds(pl.multiple_of((k * places + place) * size, 128), size)

    def ahead(d):
        return lax.rem(l + d, places)

    def behind(d):
        return lax.rem(l + places - d, places)

    def outward(k, d):
        return pltpu.make_async_remote_copy(
            src_ref=picked_ref.at[:, part(k, ahead(d))],
            dst_ref=inbox.at[:, part(k, l)],
            send_sem=send_out.at[k * places + d],
            recv_sem=recv_out.at[k * places + d],
            device_id=(g + k - 1, ahead(d)),
            device_id_type=MESH,
        )

    def homeward(k, d):
        return pltpu.make_async_remote_copy(
            src_ref=reply.at[:, part(k, behind(d))],
            dst_ref=back.at[:, part(k, l)],
            send_sem=send_back.at[k * places + d],
            recv_sem=recv_back.at[k * places + d],
            device_id=(g - k + 1, behind(d)),
            device_id_type=MESH,
        )

    def outward_in(k, d):
        return pltpu.make_async_remote_copy(
            src_ref=picked_ref.at[:, part(k, ahead(d))],
            dst_ref=inbox.at[:, part(k, behind(d))],
            send_sem=send_out.at[k * places + d],
            recv_sem=recv_out.at[k * places + d],
            device_id=(g, l),
            device_id_type=MESH,
        )

    def homeward_in(k, d):
        return pltpu.make_async_remote_copy(
            src_ref=reply.at[:, part(k, behind(d))],
            dst_ref=back.at[:, part(k, ahead(d))],
            send_sem=send_back.at[k * places + d],
            recv_sem=recv_back.at[k * places + d],
            device_id=(g, l),
            device_id_type=MESH,
        )

    barrier = pltpu.get_barrier_semaphore()
    for k, d in peers:

        @pl.when(reach[k])
        def _():
            pl.semaphore_signal(barrier, inc=1, device_id=(g + k - 1, ahead(d)), device_id_type=MESH)

    known = sum(r.astype(I32) for r in reach)
    pl.semaphore_wait(barrier, known * places - 1)

    for k, d in reversed(peers):

        @pl.when(reach[k])
        def _():
            outward(k, d).start()

    own = part(1, l)
    inbox[:, own] = picked_ref[:, own]
    for k in (0, 2):
        whole = slice(k * places * size, (k + 1) * places * size)

        @pl.when(jnp.logical_not(heard[k]))
        def _():
            inbox[:, whole] = jnp.zeros((fields, places * size), F32)

        @pl.when(jnp.logical_not(reach[k]))
        def _():
            back[:, whole] = jnp.zeros((fields, places * size), F32)

    zero = jnp.bfloat16(0)
    within_of = iota((128, 128), 0).astype(BF16)
    for q in range(slots_all // 128):
        low = jnp.broadcast_to((owned_ref[q : q + 1, :] & 127).astype(BF16), (128, 128))
        b_ref[:, q * 128 : (q + 1) * 128] = jnp.where(low == within_of, jnp.bfloat16(1), zero)

    for k, d in peers:

        @pl.when(heard[k])
        def _():
            outward_in(k, d).wait_recv()

    for q in range(slots_all // 128):
        col = slice(q * 128, (q + 1) * 128)
        both = halves(inbox[:, col])
        which = jnp.broadcast_to((owned_ref[q : q + 1, :] >> 7).astype(BF16), (16, 128))
        for h in range(heads):
            a_ref[h * 16 : (h + 1) * 16, col] = jnp.where(which == jnp.bfloat16(h), both, zero)
    summed = lax.dot_general(a_ref[...], b_ref[...], (((1,), (1,)), ((), ())), preferred_element_type=F32)
    totals = [summed[h * 16 : h * 16 + 8] + summed[h * 16 + 8 : h * 16 + 16] for h in range(heads)]
    for q in range(slots_all // 128):
        col = slice(q * 128, (q + 1) * 128)
        owned = jnp.broadcast_to(owned_ref[q : q + 1, :], (fields, 128))
        low, which = owned & 127, owned >> 7
        total = jnp.zeros((fields, 128), F32)
        for h in range(heads):
            total = jnp.where(which == h, jnp.take_along_axis(totals[h], low, axis=1), total)
        reply[:, col] = total

    for k, d in reversed(peers):

        @pl.when(heard[k])
        def _():
            homeward(k, d).start()

    back[:, own] = reply[:, own]
    for k, d in peers:

        @pl.when(reach[k])
        def _():
            homeward_in(k, d).wait_recv()

    change_ref[...] = back[...] - picked_ref[...]
    for k, d in peers:

        @pl.when(reach[k])
        def _():
            outward(k, d).wait_send()

        @pl.when(heard[k])
        def _():
            homeward(k, d).wait_send()


SMEM = pl.BlockSpec(memory_space=pltpu.SMEM)
VMEM = pl.BlockSpec(memory_space=pltpu.VMEM)
ANY = pl.BlockSpec(memory_space=pl.ANY)


def on_device(groups, places, element_values, local_map, send_node, send_count, recv_slot):
    fields, span = element_values.shape
    slots_all = send_node.shape[1]
    slot_count = slots_all // (3 * places)
    owned = 2 * slot_count
    edge = blocks_along(span)
    local = ((SIDE - 1) * edge + 1) ** 3
    tall16 = (local + 2047) // 2048 * 16
    table = (local + 96) // 96 * 96
    lines, slot_rows = span // 128, slots_all // 128
    params = pltpu.CompilerParams(vmem_limit_bytes=48 * 1024 * 1024)
    nodes, counts = send_node[0], send_count[0]
    general = [
        pltpu.SMEM((span,), I32),
        pltpu.SMEM((slots_all,), I32),
        pltpu.VMEM((span, 128), F32),
        pltpu.VMEM((table, 128), F32),
    ]
    picked, grid, spots, meta = pl.pallas_call(
        functools.partial(assemble_kernel, edge, slot_count),
        out_shape=(
            jax.ShapeDtypeStruct((fields, slots_all), F32),
            jax.ShapeDtypeStruct((fields, span), F32),
            jax.ShapeDtypeStruct((slot_rows, 128), I32),
            jax.ShapeDtypeStruct((32,), I32),
        ),
        in_specs=[VMEM, VMEM, VMEM, SMEM, ANY, ANY],
        out_specs=(VMEM, VMEM, VMEM, SMEM),
        scratch_shapes=[
            pltpu.VMEM((32 * ROWS, 128), I32),
            pltpu.VMEM((lines, 128), I32),
            pltpu.VMEM((2 * tall16, span), BF16),
            pltpu.VMEM((128, span), BF16),
            pltpu.VMEM((lines // 2 * 16, PAIR), BF16),
        ]
        + general,
        compiler_params=params,
    )(element_values, local_map.reshape(lines, 128), nodes.reshape(slot_rows, 128), counts, local_map, nodes)
    change = pl.pallas_call(
        functools.partial(exchange_kernel, groups, places),
        out_shape=jax.ShapeDtypeStruct((fields, slots_all), F32),
        in_specs=[VMEM, VMEM],
        out_specs=VMEM,
        scratch_shapes=[pltpu.VMEM((fields, slots_all), F32)] * 3
        + [
            pltpu.VMEM((owned // 128 * 16, slots_all), BF16),
            pltpu.VMEM((128, slots_all), BF16),
        ]
        + [pltpu.SemaphoreType.DMA((3 * places,))] * 4,
        compiler_params=pltpu.CompilerParams(collective_id=0, has_side_effects=True),
    )(picked, recv_slot[0].reshape(slot_rows, 128))
    return pl.pallas_call(
        functools.partial(finish_kernel, edge, slot_count),
        out_shape=jax.ShapeDtypeStruct((fields, span), F32),
        in_specs=[VMEM, VMEM, VMEM, SMEM, SMEM, ANY, ANY, ANY],
        out_specs=VMEM,
        scratch_shapes=[
            pltpu.VMEM((fields, span), F32),
            pltpu.VMEM((lines // 2 * 16, slots_all), BF16),
            pltpu.VMEM((PAIR, slots_all), BF16),
        ]
        + general,
        compiler_params=params,
    )(change, spots, grid, meta, counts, element_values, local_map, nodes)


def solution(mesh):
    return jax.shard_map(
        functools.partial(on_device, mesh.shape["grp"], mesh.shape["loc"]),
        mesh=mesh,
        in_specs=(
            P(None, ("grp", "loc")),
            P(("grp", "loc")),
            P(("grp", "loc"), None),
            P(("grp", "loc"), None),
            P(("grp", "loc"), None),
        ),
        out_specs=P(None, ("grp", "loc")),
        check_vma=False,
    )
```

```python
import functools

import jax
import jax.numpy as jnp
from jax import lax
from jax.experimental import pallas as pl
from jax.experimental.pallas import tpu as pltpu
from jax.sharding import PartitionSpec as P

MESH = pl.DeviceIdType.MESH
F32, BF16, I32 = jnp.float32, jnp.bfloat16, jnp.int32
SIDE = 8
NODES = SIDE**3
ROWS = NODES // 128
PAIR = 256
BATCH = 32


def blocks_along(span):
    edge = round((span // NODES) ** (1 / 3))
    assert edge**3 * NODES == span and 1 < edge <= 3
    return edge


def iota(shape, axis):
    return lax.broadcasted_iota(I32, shape, axis)


def halves(x):
    high = x.astype(BF16)
    low = (x - high.astype(F32)).astype(BF16)
    return jnp.concatenate([high, low], axis=0)


def add_rows(index_ref, value_ref, table_ref):
    def step(b, carry):
        base = pl.multiple_of(b * BATCH, BATCH)
        nodes = [index_ref[base + k] for k in range(BATCH)]
        held = [table_ref[pl.ds(n, 1), :] for n in nodes]
        sums = [held[k] + value_ref[pl.ds(base + k, 1), :] for k in range(BATCH)]
        for k in range(BATCH):
            table_ref[pl.ds(nodes[k], 1), :] = sums[k]
        return carry

    lax.fori_loop(0, index_ref.shape[0] // BATCH, step, 0)


def take_rows(index_ref, table_ref, out_ref):
    def step(b, carry):
        base = pl.multiple_of(b * BATCH, BATCH)
        rows = [table_ref[pl.ds(index_ref[base + k], 1), :] for k in range(BATCH)]
        for k in range(BATCH):
            out_ref[pl.ds(base + k, 1), :] = rows[k]
        return carry

    lax.fori_loop(0, index_ref.shape[0] // BATCH, step, 0)


def to_rows(flat_ref, rows_ref):
    def step(t, carry):
        base = pl.multiple_of(t * 128, 128)
        block = flat_ref[:, pl.ds(base, 128)]
        wide = jnp.concatenate([block] * (128 // block.shape[0]), axis=0)
        rows_ref[pl.ds(base, 128), :] = wide.T
        return carry

    lax.fori_loop(0, flat_ref.shape[1] // 128, step, 0)


def from_rows(rows_ref, flat_ref, put):
    def step(t, carry):
        base = pl.multiple_of(t * 128, 128)
        put(base, rows_ref[pl.ds(base, 128), :].T[: flat_ref.shape[0]])
        return carry

    lax.fori_loop(0, flat_ref.shape[1] // 128, step, 0)


def general_table(map_hbm, value_ref, map_smem, rows_ref, table_ref):
    pltpu.sync_copy(map_hbm, map_smem)
    chunk = 96

    def clear(b, carry):
        base = pl.multiple_of(b * chunk, chunk)
        table_ref[pl.ds(base, chunk), :] = jnp.zeros((chunk, 128), F32)
        return carry

    lax.fori_loop(0, table_ref.shape[0] // chunk, clear, 0)
    to_rows(value_ref, rows_ref)
    add_rows(map_smem, rows_ref, table_ref)


def sweep(ref, edge, base=None, out=None):
    lane = iota((ref.shape[0], 128), 1)
    zero = jnp.zeros((ref.shape[0], 128), F32)

    def at(px, py, pz, row):
        return pl.ds((((px * edge + py) * edge + pz) * ROWS + row) * 128, 128)

    def line(spots_of, first, last, shift, final=False):
        held = [ref[:, s] for s in spots_of]
        for i, s in enumerate(spots_of):
            total = held[i]
            if i + 1 < edge:
                total = total + jnp.where(last, pltpu.roll(held[i + 1], shift, 1), zero)
            if i > 0:
                total = total + jnp.where(first, pltpu.roll(held[i - 1], 128 - shift, 1), zero)
            if final and base is not None:
                out[:, s] = total + base[:, s]
            else:
                ref[:, s] = total

    for py in range(edge):
        for pz in range(edge):
            for px in range(edge - 1):
                a, b = at(px, py, pz, ROWS - 1), at(px + 1, py, pz, 0)
                upper, lower = ref[:, a], ref[:, b]
                ref[:, a] = upper + jnp.where(lane >= 64, pltpu.roll(lower, 64, 1), zero)
                ref[:, b] = lower + jnp.where(lane < 64, pltpu.roll(upper, 64, 1), zero)
    y, z = (lane // SIDE) % SIDE, lane % SIDE
    for px in range(edge):
        for pz in range(edge):
            for row in range(ROWS):
                line([at(px, py, pz, row) for py in range(edge)], y == 0, y == SIDE - 1, SIDE * (SIDE - 1))
    for px in range(edge):
        for py in range(edge):
            for row in range(ROWS):
                line([at(px, py, pz, row) for pz in range(edge)], z == 0, z == SIDE - 1, SIDE - 1, True)


def find_places(lab_ref, edge):
    count = edge**3
    near, mid, far = (lab_ref[pl.ds(k, 32, stride=ROWS), :].astype(F32) for k in (0, 1, ROWS - 1))
    near_t, mid_t, far_t = near.T, mid.T, far.T
    real = (iota((32, 32), 0) < count) & (iota((32, 32), 1) < count)
    sides = (
        (near, near_t, 27, far, far_t, 91),
        (mid, mid_t, 67, mid, mid_t, 123),
        (mid, mid_t, 88, mid, mid_t, 95),
    )
    place = jnp.zeros((32, 1), F32)
    for low, low_t, i, high, high_t, j in sides:
        before = jnp.where(real & (low[:, i : i + 1] == high_t[j : j + 1, :]), 1.0, 0.0)
        before_t = jnp.where(real & (high[:, j : j + 1] == low_t[i : i + 1, :]), 1.0, 0.0)
        steps = jnp.zeros((1, 32), F32)
        if edge > 2:
            steps = jnp.sum(before_t, axis=0, keepdims=True)
        place = place * edge + jnp.sum(before * (1.0 + steps), axis=1, keepdims=True)
    hit = (iota((32, 32), 0) < count) & (place == iota((32, 32), 1).astype(F32))
    who = jnp.sum(jnp.where(hit, iota((32, 32), 0).astype(F32), 0.0), axis=0, keepdims=True)
    times = jnp.sum(jnp.where(hit, 1.0, 0.0), axis=0, keepdims=True)
    wrong = jnp.where((iota((1, 32), 1) < count) & (times != 1.0), 1, 0)
    return jnp.clip(who.astype(I32), 0, count - 1), wrong


def count_mismatches(grid_ref, edge):
    total = jnp.zeros((1, 128), I32)
    lane = iota((1, 128), 1)
    y, z = (lane // SIDE) % SIDE, lane % SIDE
    for axis, stride in enumerate((edge * edge, edge, 1)):
        rows = (edge**3 - stride) * ROWS
        start = stride * ROWS - (ROWS - 1 if axis == 0 else 0)
        inner = (iota((rows, 1), 0) // ROWS // stride) % edge < edge - 1
        if axis == 0:
            where, shift = inner & (iota((rows, 1), 0) % ROWS == ROWS - 1) & (lane < 64), 64
        elif axis == 1:
            where, shift = inner & (y == 0), 128 - SIDE * (SIDE - 1)
        else:
            where, shift = inner & (z == 0), 128 - (SIDE - 1)
        low, high = grid_ref[0:rows, :], grid_ref[start : start + rows, :]
        differ = where & (pltpu.roll(low, shift, 1) != high)
        total = total + jnp.sum(jnp.where(differ, 1, 0), axis=0, keepdims=True)
    return total


def assemble_kernel(
    edge, slot_count, value_hbm, map_hbm, node_hbm, count_hbm, map_flat, node_flat,
    grid_ref, order_ref, node_ref, flag_ref, picked_ref,
    value_ref, lab_ref, raw_ref, count_ref, sems, map_smem, node_smem, rows_ref, table_ref,
):
    count = edge**3
    lines = order_ref.shape[0]
    slot_rows = node_ref.shape[0]
    labels = pltpu.make_async_copy(map_hbm, lab_ref.at[0:lines, :], sems.at[0])
    values = pltpu.make_async_copy(value_hbm, value_ref, sems.at[1])
    nodes = pltpu.make_async_copy(node_hbm, raw_ref, sems.at[2])
    counts = pltpu.make_async_copy(count_hbm, count_ref, sems.at[3])
    for copy in (labels, values, nodes, counts):
        copy.start()
    lab_ref[lines:, :] = jnp.zeros((lab_ref.shape[0] - lines, 128), I32)
    labels.wait()
    who, wrong = find_places(lab_ref, edge)
    flag_ref[...] = jnp.zeros((8, 128), I32)
    flag_ref[0:1, 0:32] = who
    values.wait()
    for s in range(count):
        e = who[0, s]
        grid_ref[:, s * NODES : (s + 1) * NODES] = value_ref[:, pl.ds(pl.multiple_of(e * NODES, NODES), NODES)]
        for r in range(ROWS):
            order_ref[s * ROWS + r : s * ROWS + r + 1, :] = lab_ref[pl.ds(e * ROWS + r, 1), :]
    sweep(grid_ref, edge)
    bad = jnp.sum(count_mismatches(order_ref, edge)) + jnp.sum(wrong)
    nodes.wait()
    counts.wait()
    per = slot_count // 128
    row_of = iota((slot_rows, 128), 0)
    limit = jnp.zeros((slot_rows, 128), I32)
    for p in range(slot_rows // per):
        limit = jnp.where(row_of // per == p, count_ref[p], limit)
    live = (row_of % per) * 128 + iota((slot_rows, 128), 1) < limit
    node_ref[...] = jnp.where(live, raw_ref[...], -1)
    flag_ref[1:2, :] = jnp.full((1, 128), bad, I32)

    @pl.when(bad > 0)
    def _():
        general_table(map_flat, value_ref, map_smem, rows_ref, table_ref)
        pltpu.sync_copy(node_flat, node_smem)
        take_rows(node_smem, table_ref, rows_ref)

        def put(base, block):
            p = base // slot_count
            keep = base - p * slot_count + iota((8, 128), 1) < count_ref[p]
            picked_ref[:, pl.ds(base, 128)] = jnp.where(keep, block, 0.0)

        from_rows(rows_ref, picked_ref, put)


def finish_kernel(
    edge, slot_count, delta_in, grid_ref, flag_ref, change_ref, count_hbm, value_hbm, map_flat, node_flat,
    out_hbm,
    delta_ref, flags, count_ref, sems, map_smem, node_smem, rows_ref, table_ref,
):
    count = edge**3
    slots_all = change_ref.shape[1]
    marks = pltpu.make_async_copy(flag_ref, flags, sems.at[0])
    marks.start()
    sweep(delta_in, edge, grid_ref, delta_ref)
    marks.wait()
    copies = []
    for s in range(count):
        spot = pl.ds(pl.multiple_of(flags[0, s] * NODES, NODES), NODES)
        copy = pltpu.make_async_copy(delta_ref.at[:, s * NODES : (s + 1) * NODES], out_hbm.at[:, spot], sems.at[1])
        copy.start()
        copies.append(copy)
    pltpu.make_async_copy(delta_ref, out_hbm, sems.at[1]).wait()

    @pl.when(flags[1, 0] > 0)
    def _():
        pltpu.sync_copy(value_hbm, delta_ref)
        pltpu.sync_copy(count_hbm, count_ref)
        general_table(map_flat, delta_ref, map_smem, rows_ref, table_ref)
        pltpu.sync_copy(node_flat, node_smem)
        to_rows(change_ref, rows_ref)
        spare = table_ref.shape[0] - 1

        def bury(i, carry):
            p = i // slot_count
            node_smem[i] = jnp.where(i - p * slot_count < count_ref[p], node_smem[i], spare)
            return carry

        lax.fori_loop(0, slots_all, bury, 0)
        add_rows(node_smem, rows_ref, table_ref)
        take_rows(map_smem, table_ref, rows_ref)

        def put(base, block):
            delta_ref[:, pl.ds(base, 128)] = block

        from_rows(rows_ref, delta_ref, put)
        pltpu.sync_copy(delta_ref, out_hbm)


def find_nodes(edge, order_ref, a_ref, b_ref):
    lines = order_ref.shape[0]
    tall16 = a_ref.shape[0] // 2
    lane = iota((1, 128), 1)
    first = (lane >= 64, (lane // SIDE) % SIDE > 0, lane % SIDE > 0)
    high_of = iota((tall16, 128), 0).astype(BF16)
    low_of = iota((128, 128), 0).astype(BF16)
    zero = jnp.bfloat16(0)
    for r in range(lines):
        s = r // ROWS
        place = (s // (edge * edge), (s // edge) % edge, s % edge)
        label = order_ref[r : r + 1, :]
        for axis in range(3):
            if place[axis] > 0 and (axis > 0 or r % ROWS == 0):
                label = jnp.where(first[axis], label, -1)
        high = jnp.broadcast_to((label >> 7).astype(BF16), (tall16, 128))
        low = jnp.broadcast_to((label & 127).astype(BF16), (128, 128))
        col = slice(r * 128, (r + 1) * 128)
        within = jnp.broadcast_to((lane + (r % 2) * 128).astype(BF16), (tall16, 128))
        hit = high == high_of
        a_ref[0:tall16, col] = jnp.where(hit, jnp.bfloat16(r // 2), zero)
        a_ref[tall16:, col] = jnp.where(hit, within, zero)
        b_ref[:, col] = jnp.where(low == low_of, jnp.bfloat16(1), zero)
    found = lax.dot_general(a_ref[...], b_ref[...], (((1,), (1,)), ((), ())), preferred_element_type=F32)
    return found[0:tall16] * PAIR + found[tall16:]


def exchange_kernel(
    groups, places, edge, order_ref, grid_ref, node_ref, owned_ref, flag_ref, other_ref,
    delta_ref, change_ref,
    picked, inbox, reply, back, spot_ref, pa_ref, pb_ref, u_ref, ta_ref, tb_ref, sa_ref, sb_ref,
    send_out, recv_out, send_back, recv_back,
):
    fields, slots_all = change_ref.shape
    size = slots_all // (3 * places)
    heads = ta_ref.shape[0] // 16
    slot_rows = node_ref.shape[0]
    blocks = grid_ref.shape[1] // PAIR
    g, l = lax.axis_index("grp"), lax.axis_index("loc")
    hops = [s * d for d in range(places - 1, 0, -1) for s in (1, -1)] + [0]
    peers = [(k, d) for d in hops for k in (0, 2, 1) if (k, d) != (1, 0)]
    reach = {(k, d): (g + k - 1 >= 0) & (g + k - 1 < groups) & (l + d >= 0) & (l + d < places) for k, d in peers}
    heard = {(k, d): (g - k + 1 >= 0) & (g - k + 1 < groups) & (l - d >= 0) & (l - d < places) for k, d in peers}

    def part(k, place):
        return pl.ds(pl.multiple_of((k * places + place) * size, 128), size)

    def copy(k, d, src, dst, near, far, sems, device):
        index = k * (2 * places - 1) + d + places - 1
        return pltpu.make_async_remote_copy(
            src_ref=src.at[:, part(k, near)],
            dst_ref=dst.at[:, part(k, far)],
            send_sem=sems[0].at[index],
            recv_sem=sems[1].at[index],
            device_id=device,
            device_id_type=MESH,
        )

    out_sems, back_sems = (send_out, recv_out), (send_back, recv_back)
    barrier = pltpu.get_barrier_semaphore()
    known = jnp.int32(0)
    for k, d in peers:
        known = known + reach[k, d].astype(I32)

        @pl.when(reach[k, d])
        def _():
            pl.semaphore_signal(barrier, inc=1, device_id=(g + k - 1, l + d), device_id_type=MESH)

    zero = jnp.bfloat16(0)
    where_is = find_nodes(edge, order_ref, pa_ref, pb_ref)
    for r in range(blocks):
        u_ref[r * 16 : (r + 1) * 16, :] = halves(grid_ref[:, r * PAIR : (r + 1) * PAIR])
    node = node_ref[...]
    high, low = node >> 7, node & 127
    spot = jnp.full((slot_rows, 128), -float(PAIR), F32)
    for h in range((((SIDE - 1) * edge + 1) ** 3 + 127) // 128):
        row = jnp.broadcast_to(where_is[h : h + 1, :], (slot_rows, 128))
        spot = jnp.where(high == h, jnp.take_along_axis(row, low, axis=1), spot)
    spot_ref[...] = spot.astype(I32)
    within_of = iota((PAIR, PAIR), 0).astype(BF16)
    block_of = iota((blocks, 1, PAIR), 0)
    general = jnp.concatenate([flag_ref[1:2, :]] * (PAIR // 128), axis=1) > 0
    for n in range(slots_all // PAIR):
        col = slice(n * PAIR, (n + 1) * PAIR)
        spots = jnp.concatenate([spot_ref[2 * n : 2 * n + 1, :], spot_ref[2 * n + 1 : 2 * n + 2, :]], axis=1)
        low = jnp.broadcast_to((spots & (PAIR - 1)).astype(BF16), (PAIR, PAIR))
        onehot = jnp.where(low == within_of, jnp.bfloat16(1), zero)
        both = jnp.dot(u_ref[...], onehot, preferred_element_type=F32)
        which = jnp.broadcast_to(spots >> 8, (fields, PAIR))
        top = jnp.zeros((fields, PAIR), F32)
        rest = jnp.zeros((fields, PAIR), F32)
        for r in range(blocks):
            mine = which == r
            top = jnp.where(mine, both[r * 16 : r * 16 + 8], top)
            rest = jnp.where(mine, both[r * 16 + 8 : r * 16 + 16], rest)
        picked[:, col] = jnp.where(general, other_ref[:, col], top + rest)

    pl.semaphore_wait(barrier, known)
    for k, d in peers:

        @pl.when(reach[k, d])
        def _():
            copy(k, d, picked, inbox, l + d, l, out_sems, (g + k - 1, l + d)).start()

    own = part(1, l)
    inbox[:, own] = picked[:, own]
    for k in (0, 2):
        whole = slice(k * places * size, (k + 1) * places * size)

        @pl.when(jnp.logical_not(heard[k, 0]))
        def _():
            inbox[:, whole] = jnp.zeros((fields, places * size), F32)

        @pl.when(jnp.logical_not(reach[k, 0]))
        def _():
            back[:, whole] = jnp.zeros((fields, places * size), F32)

    owned_low = iota((128, 128), 0).astype(BF16)
    spot_low = iota((PAIR, 128), 0).astype(BF16)
    for q in range(slots_all // 128):
        col = slice(q * 128, (q + 1) * 128)
        low = jnp.broadcast_to((owned_ref[q : q + 1, :] & 127).astype(BF16), (128, 128))
        tb_ref[:, col] = jnp.where(low == owned_low, jnp.bfloat16(1), zero)
        low = jnp.broadcast_to((spot_ref[q : q + 1, :] & (PAIR - 1)).astype(BF16), (PAIR, 128))
        sb_ref[:, col] = jnp.where(low == spot_low, jnp.bfloat16(1), zero)

    for k, d in reversed(peers):

        @pl.when(heard[k, d])
        def _():
            copy(k, d, picked, inbox, l, l - d, out_sems, (g, l)).wait_recv()

    for q in range(slots_all // 128):
        col = slice(q * 128, (q + 1) * 128)
        both = halves(inbox[:, col])
        which = jnp.broadcast_to((owned_ref[q : q + 1, :] >> 7).astype(BF16), (16, 128))
        for h in range(heads):
            ta_ref[h * 16 : (h + 1) * 16, col] = jnp.where(which == jnp.bfloat16(h), both, zero)
    summed = lax.dot_general(ta_ref[...], tb_ref[...], (((1,), (1,)), ((), ())), preferred_element_type=F32)
    totals = [summed[h * 16 : h * 16 + 8] + summed[h * 16 + 8 : h * 16 + 16] for h in range(heads)]
    for q in range(slots_all // 128):
        col = slice(q * 128, (q + 1) * 128)
        owned = jnp.broadcast_to(owned_ref[q : q + 1, :], (fields, 128))
        low, which = owned & 127, owned >> 7
        total = jnp.zeros((fields, 128), F32)
        for h in range(heads):
            total = jnp.where(which == h, jnp.take_along_axis(totals[h], low, axis=1), total)
        reply[:, col] = total

    for k, d in peers:

        @pl.when(heard[k, d])
        def _():
            copy(k, d, reply, back, l - d, l, back_sems, (g - k + 1, l - d)).start()

    back[:, own] = reply[:, own]
    for k, d in reversed(peers):

        @pl.when(reach[k, d])
        def _():
            copy(k, d, reply, back, l, l + d, back_sems, (g, l)).wait_recv()

    for q in range(slots_all // 128):
        col = slice(q * 128, (q + 1) * 128)
        change = back[:, col] - picked[:, col]
        change_ref[:, col] = change
        both = halves(change)
        which = jnp.broadcast_to((spot_ref[q : q + 1, :] >> 8).astype(BF16), (16, 128))
        for r in range(blocks):
            sa_ref[r * 16 : (r + 1) * 16, col] = jnp.where(which == jnp.bfloat16(r), both, zero)
    spread = lax.dot_general(sa_ref[...], sb_ref[...], (((1,), (1,)), ((), ())), preferred_element_type=F32)
    for r in range(blocks):
        delta_ref[:, r * PAIR : (r + 1) * PAIR] = spread[r * 16 : r * 16 + 8] + spread[r * 16 + 8 : r * 16 + 16]

    for k, d in peers:

        @pl.when(reach[k, d])
        def _():
            copy(k, d, picked, inbox, l + d, l, out_sems, (g, l)).wait_send()

        @pl.when(heard[k, d])
        def _():
            copy(k, d, reply, back, l - d, l, back_sems, (g, l)).wait_send()


SMEM = pl.BlockSpec(memory_space=pltpu.SMEM)
VMEM = pl.BlockSpec(memory_space=pltpu.VMEM)
HBM = pl.BlockSpec(memory_space=pltpu.HBM)


def on_device(groups, places, element_values, local_map, send_node, send_count, recv_slot):
    fields, span = element_values.shape
    slots_all = send_node.shape[1]
    slot_count = slots_all // (3 * places)
    owned = 2 * slot_count
    edge = blocks_along(span)
    local = ((SIDE - 1) * edge + 1) ** 3
    tall16 = (local + 2047) // 2048 * 16
    table = (local + 96) // 96 * 96
    lines, slot_rows = span // 128, slots_all // 128
    map_rows, node_rows = local_map.reshape(-1, 128), send_node.reshape(-1, 128)
    owned_rows = recv_slot.reshape(-1, 128)
    element_values, local_map, map_rows, node_rows, nodes, counts = (
        pltpu.with_memory_space_constraint(x, pltpu.HBM)
        for x in (element_values, local_map, map_rows, node_rows, send_node.reshape(-1), send_count.reshape(-1))
    )
    shape = jax.ShapeDtypeStruct
    general = [
        pltpu.SMEM((span,), I32),
        pltpu.SMEM((slots_all,), I32),
        pltpu.VMEM((span, 128), F32),
        pltpu.VMEM((table, 128), F32),
    ]
    grid, order, live_nodes, flags, other = pl.pallas_call(
        functools.partial(assemble_kernel, edge, slot_count),
        out_shape=(
            shape((fields, span), F32),
            shape((lines, 128), I32),
            shape((slot_rows, 128), I32),
            shape((8, 128), I32),
            shape((fields, slots_all), F32),
        ),
        in_specs=[HBM] * 6,
        out_specs=(VMEM,) * 5,
        scratch_shapes=[
            pltpu.VMEM((fields, span), F32),
            pltpu.VMEM((32 * ROWS, 128), I32),
            pltpu.VMEM((slot_rows, 128), I32),
            pltpu.SMEM(counts.shape, I32),
            pltpu.SemaphoreType.DMA((4,)),
        ]
        + general,
        compiler_params=pltpu.CompilerParams(vmem_limit_bytes=24 * 1024 * 1024),
    )(element_values, map_rows, node_rows, counts, local_map, nodes)
    delta, change = pl.pallas_call(
        functools.partial(exchange_kernel, groups, places, edge),
        out_shape=(shape((fields, span), F32), shape((fields, slots_all), F32)),
        in_specs=[VMEM] * 6,
        out_specs=(VMEM, VMEM),
        scratch_shapes=[pltpu.VMEM((fields, slots_all), F32)] * 4
        + [
            pltpu.VMEM((slot_rows, 128), I32),
            pltpu.VMEM((2 * tall16, span), BF16),
            pltpu.VMEM((128, span), BF16),
            pltpu.VMEM((lines // 2 * 16, PAIR), BF16),
            pltpu.VMEM((owned // 128 * 16, slots_all), BF16),
            pltpu.VMEM((128, slots_all), BF16),
            pltpu.VMEM((lines // 2 * 16, slots_all), BF16),
            pltpu.VMEM((PAIR, slots_all), BF16),
        ]
        + [pltpu.SemaphoreType.DMA((3 * (2 * places - 1),))] * 4,
        compiler_params=pltpu.CompilerParams(
            collective_id=0, has_side_effects=True, vmem_limit_bytes=40 * 1024 * 1024
        ),
    )(order, grid, live_nodes, owned_rows, flags, other)
    return pl.pallas_call(
        functools.partial(finish_kernel, edge, slot_count),
        out_shape=shape((fields, span), F32),
        in_specs=[VMEM] * 4 + [HBM] * 4,
        out_specs=HBM,
        scratch_shapes=[
            pltpu.VMEM((fields, span), F32),
            pltpu.SMEM((8, 128), I32),
            pltpu.SMEM(counts.shape, I32),
            pltpu.SemaphoreType.DMA((2,)),
        ]
        + general,
        compiler_params=pltpu.CompilerParams(vmem_limit_bytes=24 * 1024 * 1024),
    )(delta, grid, flags, change, counts, element_values, local_map, nodes)


def solution(mesh):
    return jax.shard_map(
        functools.partial(on_device, mesh.shape["grp"], mesh.shape["loc"]),
        mesh=mesh,
        in_specs=(
            P(None, ("grp", "loc")),
            P(("grp", "loc")),
            P(("grp", "loc"), None),
            P(("grp", "loc"), None),
            P(("grp", "loc"), None),
        ),
        out_specs=P(None, ("grp", "loc")),
        check_vma=False,
    )
```

```python
import functools

import jax
import jax.numpy as jnp
from jax import lax
from jax.experimental import pallas as pl
from jax.experimental.pallas import tpu as pltpu
from jax.sharding import PartitionSpec as P

MESH = pl.DeviceIdType.MESH
F32, BF16, I32 = jnp.float32, jnp.bfloat16, jnp.int32
SIDE = 8
NODES = SIDE**3
ROWS = NODES // 128
PAIR = 256
BATCH = 32


def blocks_along(span):
    edge = round((span // NODES) ** (1 / 3))
    assert edge**3 * NODES == span and 1 < edge <= 3
    return edge


def iota(shape, axis):
    return lax.broadcasted_iota(I32, shape, axis)


def halves(x):
    high = x.astype(BF16)
    low = (x - high.astype(F32)).astype(BF16)
    return jnp.concatenate([high, low], axis=0)


def add_rows(index_ref, value_ref, table_ref):
    def step(b, carry):
        base = pl.multiple_of(b * BATCH, BATCH)
        nodes = [index_ref[base + k] for k in range(BATCH)]
        held = [table_ref[pl.ds(n, 1), :] for n in nodes]
        sums = [held[k] + value_ref[pl.ds(base + k, 1), :] for k in range(BATCH)]
        for k in range(BATCH):
            table_ref[pl.ds(nodes[k], 1), :] = sums[k]
        return carry

    lax.fori_loop(0, index_ref.shape[0] // BATCH, step, 0)


def take_rows(index_ref, table_ref, out_ref):
    def step(b, carry):
        base = pl.multiple_of(b * BATCH, BATCH)
        rows = [table_ref[pl.ds(index_ref[base + k], 1), :] for k in range(BATCH)]
        for k in range(BATCH):
            out_ref[pl.ds(base + k, 1), :] = rows[k]
        return carry

    lax.fori_loop(0, index_ref.shape[0] // BATCH, step, 0)


def to_rows(flat_ref, rows_ref):
    def step(t, carry):
        base = pl.multiple_of(t * 128, 128)
        block = flat_ref[:, pl.ds(base, 128)]
        wide = jnp.concatenate([block] * (128 // block.shape[0]), axis=0)
        rows_ref[pl.ds(base, 128), :] = wide.T
        return carry

    lax.fori_loop(0, flat_ref.shape[1] // 128, step, 0)


def from_rows(rows_ref, flat_ref, put):
    def step(t, carry):
        base = pl.multiple_of(t * 128, 128)
        put(base, rows_ref[pl.ds(base, 128), :].T[: flat_ref.shape[0]])
        return carry

    lax.fori_loop(0, flat_ref.shape[1] // 128, step, 0)


def general_table(map_hbm, value_ref, map_smem, rows_ref, table_ref):
    pltpu.sync_copy(map_hbm, map_smem)
    chunk = 96

    def clear(b, carry):
        base = pl.multiple_of(b * chunk, chunk)
        table_ref[pl.ds(base, chunk), :] = jnp.zeros((chunk, 128), F32)
        return carry

    lax.fori_loop(0, table_ref.shape[0] // chunk, clear, 0)
    to_rows(value_ref, rows_ref)
    add_rows(map_smem, rows_ref, table_ref)


def sweep(ref, edge, base=None, out=None):
    lane = iota((ref.shape[0], 128), 1)
    zero = jnp.zeros((ref.shape[0], 128), F32)

    def at(px, py, pz, row):
        return pl.ds((((px * edge + py) * edge + pz) * ROWS + row) * 128, 128)

    def line(spots_of, first, last, shift, final=False):
        held = [ref[:, s] for s in spots_of]
        for i, s in enumerate(spots_of):
            total = held[i]
            if i + 1 < edge:
                total = total + jnp.where(last, pltpu.roll(held[i + 1], shift, 1), zero)
            if i > 0:
                total = total + jnp.where(first, pltpu.roll(held[i - 1], 128 - shift, 1), zero)
            if final and base is not None:
                out[:, s] = total + base[:, s]
            else:
                ref[:, s] = total

    for py in range(edge):
        for pz in range(edge):
            for px in range(edge - 1):
                a, b = at(px, py, pz, ROWS - 1), at(px + 1, py, pz, 0)
                upper, lower = ref[:, a], ref[:, b]
                ref[:, a] = upper + jnp.where(lane >= 64, pltpu.roll(lower, 64, 1), zero)
                ref[:, b] = lower + jnp.where(lane < 64, pltpu.roll(upper, 64, 1), zero)
    y, z = (lane // SIDE) % SIDE, lane % SIDE
    for px in range(edge):
        for pz in range(edge):
            for row in range(ROWS):
                line([at(px, py, pz, row) for py in range(edge)], y == 0, y == SIDE - 1, SIDE * (SIDE - 1))
        for py in range(edge):
            for row in range(ROWS):
                line([at(px, py, pz, row) for pz in range(edge)], z == 0, z == SIDE - 1, SIDE - 1, True)


def find_places(lab_ref, edge):
    count = edge**3
    near, mid, far = (lab_ref[pl.ds(k, 32, stride=ROWS), :].astype(F32) for k in (0, 1, ROWS - 1))
    near_t, mid_t, far_t = near.T, mid.T, far.T
    real = (iota((32, 32), 0) < count) & (iota((32, 32), 1) < count)
    sides = (
        (near, near_t, 27, far, far_t, 91),
        (mid, mid_t, 67, mid, mid_t, 123),
        (mid, mid_t, 88, mid, mid_t, 95),
    )
    place = jnp.zeros((32, 1), F32)
    for low, low_t, i, high, high_t, j in sides:
        before = jnp.where(real & (low[:, i : i + 1] == high_t[j : j + 1, :]), 1.0, 0.0)
        before_t = jnp.where(real & (high[:, j : j + 1] == low_t[i : i + 1, :]), 1.0, 0.0)
        steps = jnp.zeros((1, 32), F32)
        if edge > 2:
            steps = jnp.sum(before_t, axis=0, keepdims=True)
        place = place * edge + jnp.sum(before * (1.0 + steps), axis=1, keepdims=True)
    hit = (iota((32, 32), 0) < count) & (place == iota((32, 32), 1).astype(F32))
    who = jnp.sum(jnp.where(hit, iota((32, 32), 0).astype(F32), 0.0), axis=0, keepdims=True)
    times = jnp.sum(jnp.where(hit, 1.0, 0.0), axis=0, keepdims=True)
    wrong = jnp.where((iota((1, 32), 1) < count) & (times != 1.0), 1, 0)
    return jnp.clip(who.astype(I32), 0, count - 1), wrong


def count_mismatches(grid_ref, edge):
    total = jnp.zeros((1, 128), I32)
    lane = iota((1, 128), 1)
    y, z = (lane // SIDE) % SIDE, lane % SIDE
    for axis, stride in enumerate((edge * edge, edge, 1)):
        rows = (edge**3 - stride) * ROWS
        start = stride * ROWS - (ROWS - 1 if axis == 0 else 0)
        inner = (iota((rows, 1), 0) // ROWS // stride) % edge < edge - 1
        if axis == 0:
            where, shift = inner & (iota((rows, 1), 0) % ROWS == ROWS - 1) & (lane < 64), 64
        elif axis == 1:
            where, shift = inner & (y == 0), 128 - SIDE * (SIDE - 1)
        else:
            where, shift = inner & (z == 0), 128 - (SIDE - 1)
        low, high = grid_ref[0:rows, :], grid_ref[start : start + rows, :]
        differ = where & (pltpu.roll(low, shift, 1) != high)
        total = total + jnp.sum(jnp.where(differ, 1, 0), axis=0, keepdims=True)
    return total


def order_kernel(
    edge, slot_count, map_hbm, node_hbm, count_hbm, value_hbm, map_flat, node_flat,
    order_ref, node_ref, flag_ref, picked_ref, grid_ref,
    lab_ref, raw_ref, count_ref, sems, value_ref, map_smem, node_smem, rows_ref, table_ref,
):
    count = edge**3
    lines = order_ref.shape[0]
    slot_rows = node_ref.shape[0]
    labels = pltpu.make_async_copy(map_hbm, lab_ref.at[0:lines, :], sems.at[0])
    nodes = pltpu.make_async_copy(node_hbm, raw_ref, sems.at[1])
    counts = pltpu.make_async_copy(count_hbm, count_ref, sems.at[2])
    values = pltpu.make_async_copy(value_hbm, value_ref, sems.at[3])
    for copy in (labels, nodes, counts, values):
        copy.start()
    lab_ref[lines:, :] = jnp.zeros((lab_ref.shape[0] - lines, 128), I32)
    labels.wait()
    who, wrong = find_places(lab_ref, edge)
    flag_ref[...] = jnp.zeros((8, 128), I32)
    flag_ref[0:1, 0:32] = who
    values.wait()
    for s in range(count):
        e = who[0, s]
        grid_ref[:, s * NODES : (s + 1) * NODES] = value_ref[:, pl.ds(pl.multiple_of(e * NODES, NODES), NODES)]
        for r in range(ROWS):
            order_ref[s * ROWS + r : s * ROWS + r + 1, :] = lab_ref[pl.ds(e * ROWS + r, 1), :]
    bad = jnp.sum(count_mismatches(order_ref, edge)) + jnp.sum(wrong)
    nodes.wait()
    counts.wait()
    per = slot_count // 128
    row_of = iota((slot_rows, 128), 0)
    limit = jnp.zeros((slot_rows, 128), I32)
    for p in range(slot_rows // per):
        limit = jnp.where(row_of // per == p, count_ref[p], limit)
    live = (row_of % per) * 128 + iota((slot_rows, 128), 1) < limit
    node_ref[...] = jnp.where(live, raw_ref[...], -1)
    flag_ref[1:2, :] = jnp.full((1, 128), bad, I32)

    @pl.when(bad > 0)
    def _():
        general_table(map_flat, value_ref, map_smem, rows_ref, table_ref)
        pltpu.sync_copy(node_flat, node_smem)
        take_rows(node_smem, table_ref, rows_ref)

        def put(base, block):
            p = base // slot_count
            keep = base - p * slot_count + iota((8, 128), 1) < count_ref[p]
            picked_ref[:, pl.ds(base, 128)] = jnp.where(keep, block, 0.0)

        from_rows(rows_ref, picked_ref, put)


def finish_kernel(
    edge, slot_count, delta_in, grid_ref, flag_ref, change_ref, count_hbm, value_hbm, map_flat, node_flat,
    out_hbm,
    delta_ref, flags, count_ref, sems, map_smem, node_smem, rows_ref, table_ref,
):
    count = edge**3
    slots_all = change_ref.shape[1]
    marks = pltpu.make_async_copy(flag_ref, flags, sems.at[0])
    marks.start()
    sweep(delta_in, edge, grid_ref, delta_ref)
    marks.wait()
    for s in range(count):
        spot = pl.ds(pl.multiple_of(flags[0, s] * NODES, NODES), NODES)
        pltpu.make_async_copy(delta_ref.at[:, s * NODES : (s + 1) * NODES], out_hbm.at[:, spot], sems.at[1]).start()
    pltpu.make_async_copy(delta_ref, out_hbm, sems.at[1]).wait()

    @pl.when(flags[1, 0] > 0)
    def _():
        pltpu.sync_copy(value_hbm, delta_ref)
        pltpu.sync_copy(count_hbm, count_ref)
        general_table(map_flat, delta_ref, map_smem, rows_ref, table_ref)
        pltpu.sync_copy(node_flat, node_smem)
        to_rows(change_ref, rows_ref)
        spare = table_ref.shape[0] - 1

        def bury(i, carry):
            p = i // slot_count
            node_smem[i] = jnp.where(i - p * slot_count < count_ref[p], node_smem[i], spare)
            return carry

        lax.fori_loop(0, slots_all, bury, 0)
        add_rows(node_smem, rows_ref, table_ref)
        take_rows(map_smem, table_ref, rows_ref)

        def put(base, block):
            delta_ref[:, pl.ds(base, 128)] = block

        from_rows(rows_ref, delta_ref, put)
        pltpu.sync_copy(delta_ref, out_hbm)


def find_nodes(edge, order_ref, a_ref, b_ref):
    lines = order_ref.shape[0]
    tall16 = a_ref.shape[0] // 2
    lane = iota((1, 128), 1)
    first = (lane >= 64, (lane // SIDE) % SIDE > 0, lane % SIDE > 0)
    high_of = iota((tall16, 128), 0).astype(BF16)
    low_of = iota((128, 128), 0).astype(BF16)
    zero = jnp.bfloat16(0)
    for r in range(lines):
        s = r // ROWS
        place = (s // (edge * edge), (s // edge) % edge, s % edge)
        label = order_ref[r : r + 1, :]
        for axis in range(3):
            if place[axis] > 0 and (axis > 0 or r % ROWS == 0):
                label = jnp.where(first[axis], label, -1)
        high = jnp.broadcast_to((label >> 7).astype(BF16), (tall16, 128))
        low = jnp.broadcast_to((label & 127).astype(BF16), (128, 128))
        col = slice(r * 128, (r + 1) * 128)
        within = jnp.broadcast_to((lane + (r % 2) * 128).astype(BF16), (tall16, 128))
        hit = high == high_of
        a_ref[0:tall16, col] = jnp.where(hit, jnp.bfloat16(r // 2), zero)
        a_ref[tall16:, col] = jnp.where(hit, within, zero)
        b_ref[:, col] = jnp.where(low == low_of, jnp.bfloat16(1), zero)
    found = lax.dot_general(a_ref[...], b_ref[...], (((1,), (1,)), ((), ())), preferred_element_type=F32)
    return found[0:tall16] * PAIR + found[tall16:]


def exchange_kernel(
    groups, places, edge, order_ref, node_ref, owned_ref, flag_ref, other_ref, raw_ref,
    grid_ref, delta_ref, change_ref,
    picked, inbox, reply, back, spot_ref, pa_ref, pb_ref, u_ref, ta_ref, tb_ref, sa_ref, sb_ref,
    send_out, recv_out, send_back, recv_back,
):
    fields, slots_all = change_ref.shape
    size = slots_all // (3 * places)
    heads = ta_ref.shape[0] // 16
    blocks = grid_ref.shape[1] // PAIR
    g, l = lax.axis_index("grp"), lax.axis_index("loc")

    far = [jnp.where(m > l, m - l, l - m) for m in range(places)]
    rank = [
        sum(((far[n] > far[m]) | ((far[n] == far[m]) & (n > m))).astype(I32) for n in range(places) if n != m)
        for m in range(places)
    ]
    places_by = [sum(jnp.where(rank[m] == i, m, 0) for m in range(places)) for i in range(places - 1)] + [l]

    def group(k):
        return lax.rem(g + groups + k, groups)

    def others(i):
        return (0, 2) if i == places - 1 else (0, 2, 1)

    def part(k, place):
        return pl.ds(pl.multiple_of((k * places + place) * size, 128), size)

    def lines_of(k, place):
        return [pl.ds((k * places + place) * (size // 128) + j, 1) for j in range(size // 128)]

    def copy(k, src, dst, there, near, sems, device):
        return pltpu.make_async_remote_copy(
            src_ref=src.at[:, part(k, there)],
            dst_ref=dst.at[:, part(k, near)],
            send_sem=sems[0].at[k * places + there],
            recv_sem=sems[1].at[k * places + near],
            device_id=device,
            device_id_type=MESH,
        )

    def outward(k, m):
        return copy(k, picked, inbox, m, l, (send_out, recv_out), (group(k - 1), m))

    def inward(k, m):
        return copy(k, picked, inbox, m, m, (send_out, recv_out), (group(1 - k), m))

    def homeward(k, m):
        return copy(k, reply, back, m, l, (send_back, recv_back), (group(1 - k), m))

    def returned(k, m):
        return copy(k, reply, back, m, m, (send_back, recv_back), (group(k - 1), m))

    barrier = pltpu.get_barrier_semaphore()
    for i in range(places):
        for k in others(i):
            pl.semaphore_signal(barrier, inc=1, device_id=(group(k - 1), places_by[i]), device_id_type=MESH)

    zero = jnp.bfloat16(0)
    where_is = find_nodes(edge, order_ref, pa_ref, pb_ref)
    grid_ref[...] = raw_ref[...]
    sweep(grid_ref, edge)
    for r in range(blocks):
        u_ref[r * 16 : (r + 1) * 16, :] = halves(grid_ref[:, r * PAIR : (r + 1) * PAIR])
    delta_ref[...] = jnp.zeros(delta_ref.shape, F32)

    def spots_of(k, i):
        row = i * (spot_ref.shape[0] // places) + k * (size // 128)
        return jnp.concatenate([spot_ref[row + j : row + j + 1, :] for j in range(size // 128)], axis=1)

    def owned_of(k, m):
        return jnp.concatenate([owned_ref[line, :] for line in lines_of(k, m)], axis=1)

    def onehot(index, count):
        low = jnp.broadcast_to((index & (count - 1)).astype(BF16), (count, size))
        return jnp.where(low == iota((count, size), 0).astype(BF16), jnp.bfloat16(1), zero)

    tall = (((SIDE - 1) * edge + 1) ** 3 + 127) // 128

    def look_up(i, m):
        rows = [line for k in range(3) for line in lines_of(k, m)]
        spare = [jnp.full((8 - len(rows) % 8, 128), -1, I32)] if len(rows) % 8 else []
        node = jnp.concatenate([node_ref[line, :] for line in rows] + spare, axis=0)
        high, low = node >> 7, node & 127
        spot = jnp.full(node.shape, -float(PAIR), F32)
        for h in range(tall):
            row = jnp.broadcast_to(where_is[h : h + 1, :], node.shape)
            spot = jnp.where(high == h, jnp.take_along_axis(row, low, axis=1), spot)
        spot_ref[i * spot.shape[0] : (i + 1) * spot.shape[0], :] = spot.astype(I32)

    def pick_by_lane(spots):
        parts = []
        for j in range(size // 128):
            index = jnp.broadcast_to(spots[:, j * 128 : (j + 1) * 128], (fields, 128))
            which, low = index >> 7, index & 127
            value = jnp.zeros((fields, 128), F32)
            for r in range(2 * blocks):
                held = jnp.take_along_axis(grid_ref[:, r * 128 : (r + 1) * 128], low, axis=1)
                value = jnp.where(which == r, held, value)
            parts.append(value)
        return jnp.concatenate(parts, axis=1)

    general = jnp.concatenate([flag_ref[1:2, :]] * (size // 128), axis=1) > 0
    for i in range(places):
        m = places_by[i]
        look_up(i, m)
        by_lane = pick_by_lane(spots_of(1, i))
        picked[:, part(1, m)] = jnp.where(general, other_ref[:, part(1, m)], by_lane)
        for k in (0, 2):
            spots = spots_of(k, i)
            both = jnp.dot(u_ref[...], onehot(spots, PAIR), preferred_element_type=F32)
            which = jnp.broadcast_to(spots >> 8, (fields, size))
            top = jnp.zeros((fields, size), F32)
            rest = jnp.zeros((fields, size), F32)
            for r in range(blocks):
                mine = which == r
                top = jnp.where(mine, both[r * 16 : r * 16 + 8], top)
                rest = jnp.where(mine, both[r * 16 + 8 : r * 16 + 16], rest)
            picked[:, part(k, m)] = jnp.where(general, other_ref[:, part(k, m)], top + rest)
        if i == 1:
            pl.semaphore_wait(barrier, 3 * places - 1)
        for n in range(0 if i == 1 else i, i + 1 if i else 0):
            for k in others(n):
                outward(k, places_by[n]).start()

    for i in range(places):
        for k in range(3):
            sb_ref[:, part(k, places_by[i])] = onehot(spots_of(k, i), PAIR)
            tb_ref[:, part(k, places_by[i])] = onehot(owned_of(k, places_by[i]), 128)
    summed = jnp.zeros((heads * 16, 128), F32)
    for i in reversed(range(places)):
        m = places_by[i]
        for k in others(i):
            inward(k, m).wait_recv()
        for k in range(3):
            source = picked if (i, k) == (places - 1, 1) else inbox
            both = halves(source[:, part(k, m)])
            which = jnp.broadcast_to((owned_of(k, m) >> 7).astype(BF16), (16, size))
            for h in range(heads):
                ta_ref[h * 16 : (h + 1) * 16, k * size : (k + 1) * size] = jnp.where(which == jnp.bfloat16(h), both, zero)
        right = jnp.concatenate([tb_ref[:, part(k, m)] for k in range(3)], axis=1)
        summed = summed + lax.dot_general(
            ta_ref[...], right, (((1,), (1,)), ((), ())), preferred_element_type=F32
        )
    totals = [summed[h * 16 : h * 16 + 8] + summed[h * 16 + 8 : h * 16 + 16] for h in range(heads)]
    for i in range(places):
        m = places_by[i]
        for k in range(3):
            owned = owned_of(k, m)
            for j in range(size // 128):
                index = jnp.broadcast_to(owned[:, j * 128 : (j + 1) * 128], (fields, 128))
                low, which = index & 127, index >> 7
                total = jnp.zeros((fields, 128), F32)
                for h in range(heads):
                    total = jnp.where(which == h, jnp.take_along_axis(totals[h], low, axis=1), total)
                reply[:, pl.ds(pl.multiple_of((k * places + m) * size + j * 128, 128), 128)] = total
        for k in others(i):
            homeward(k, m).start()

    for i in reversed(range(places)):
        m = places_by[i]
        for k in others(i):
            returned(k, m).wait_recv()
        for k in range(3):
            source = reply if (i, k) == (places - 1, 1) else back
            change = source[:, part(k, m)] - picked[:, part(k, m)]
            change_ref[:, part(k, m)] = change
            both = halves(change)
            which = jnp.broadcast_to((spots_of(k, i) >> 8).astype(BF16), (16, size))
            for r in range(blocks):
                sa_ref[r * 16 : (r + 1) * 16, k * size : (k + 1) * size] = jnp.where(which == jnp.bfloat16(r), both, zero)
        right = jnp.concatenate([sb_ref[:, part(k, m)] for k in range(3)], axis=1)
        spread = lax.dot_general(sa_ref[...], right, (((1,), (1,)), ((), ())), preferred_element_type=F32)
        for r in range(blocks):
            col = slice(r * PAIR, (r + 1) * PAIR)
            delta_ref[:, col] += spread[r * 16 : r * 16 + 8] + spread[r * 16 + 8 : r * 16 + 16]

    for i in range(places):
        for k in others(i):
            outward(k, places_by[i]).wait_send()
            homeward(k, places_by[i]).wait_send()


SMEM = pl.BlockSpec(memory_space=pltpu.SMEM)
VMEM = pl.BlockSpec(memory_space=pltpu.VMEM)
HBM = pl.BlockSpec(memory_space=pltpu.HBM)


def on_device(groups, places, element_values, local_map, send_node, send_count, recv_slot):
    fields, span = element_values.shape
    slots_all = send_node.shape[1]
    slot_count = slots_all // (3 * places)
    owned = 2 * slot_count
    edge = blocks_along(span)
    local = ((SIDE - 1) * edge + 1) ** 3
    tall16 = (local + 2047) // 2048 * 16
    table = (local + 96) // 96 * 96
    lines, slot_rows = span // 128, slots_all // 128
    map_rows, node_rows = local_map.reshape(-1, 128), send_node.reshape(-1, 128)
    owned_rows = recv_slot.reshape(-1, 128)
    element_values, local_map, map_rows, node_rows, nodes, counts = (
        pltpu.with_memory_space_constraint(x, pltpu.HBM)
        for x in (element_values, local_map, map_rows, node_rows, send_node.reshape(-1), send_count.reshape(-1))
    )
    shape = jax.ShapeDtypeStruct
    general = [
        pltpu.SMEM((span,), I32),
        pltpu.SMEM((slots_all,), I32),
        pltpu.VMEM((span, 128), F32),
        pltpu.VMEM((table, 128), F32),
    ]
    order, live_nodes, flags, other, raw = pl.pallas_call(
        functools.partial(order_kernel, edge, slot_count),
        out_shape=(
            shape((lines, 128), I32),
            shape((slot_rows, 128), I32),
            shape((8, 128), I32),
            shape((fields, slots_all), F32),
            shape((fields, span), F32),
        ),
        in_specs=[HBM] * 6,
        out_specs=(VMEM,) * 5,
        scratch_shapes=[
            pltpu.VMEM((32 * ROWS, 128), I32),
            pltpu.VMEM((slot_rows, 128), I32),
            pltpu.SMEM(counts.shape, I32),
            pltpu.SemaphoreType.DMA((4,)),
            pltpu.VMEM((fields, span), F32),
        ]
        + general,
        compiler_params=pltpu.CompilerParams(vmem_limit_bytes=24 * 1024 * 1024),
    )(map_rows, node_rows, counts, element_values, local_map, nodes)
    grid, delta, change = pl.pallas_call(
        functools.partial(exchange_kernel, groups, places, edge),
        out_shape=(shape((fields, span), F32), shape((fields, span), F32), shape((fields, slots_all), F32)),
        in_specs=[VMEM] * 6,
        out_specs=(VMEM,) * 3,
        scratch_shapes=[pltpu.VMEM((fields, slots_all), F32)] * 4
        + [
            pltpu.VMEM((places * ((3 * slot_count // 128 + 7) // 8 * 8), 128), I32),
            pltpu.VMEM((2 * tall16, span), BF16),
            pltpu.VMEM((128, span), BF16),
            pltpu.VMEM((lines // 2 * 16, PAIR), BF16),
            pltpu.VMEM((owned // 128 * 16, 3 * slot_count), BF16),
            pltpu.VMEM((128, slots_all), BF16),
            pltpu.VMEM((lines // 2 * 16, 3 * slot_count), BF16),
            pltpu.VMEM((PAIR, slots_all), BF16),
        ]
        + [pltpu.SemaphoreType.DMA((3 * places,))] * 4,
        compiler_params=pltpu.CompilerParams(
            collective_id=0, has_side_effects=True, vmem_limit_bytes=40 * 1024 * 1024
        ),
    )(order, live_nodes, owned_rows, flags, other, raw)
    return pl.pallas_call(
        functools.partial(finish_kernel, edge, slot_count),
        out_shape=shape((fields, span), F32),
        in_specs=[VMEM] * 4 + [HBM] * 4,
        out_specs=HBM,
        scratch_shapes=[
            pltpu.VMEM((fields, span), F32),
            pltpu.SMEM((8, 128), I32),
            pltpu.SMEM(counts.shape, I32),
            pltpu.SemaphoreType.DMA((2,)),
        ]
        + general,
        compiler_params=pltpu.CompilerParams(vmem_limit_bytes=24 * 1024 * 1024),
    )(delta, grid, flags, change, counts, element_values, local_map, nodes)


def solution(mesh):
    return jax.shard_map(
        functools.partial(on_device, mesh.shape["grp"], mesh.shape["loc"]),
        mesh=mesh,
        in_specs=(
            P(None, ("grp", "loc")),
            P(("grp", "loc")),
            P(("grp", "loc"), None),
            P(("grp", "loc"), None),
            P(("grp", "loc"), None),
        ),
        out_specs=P(None, ("grp", "loc")),
        check_vma=False,
    )
```

```python
import functools

import jax
import jax.numpy as jnp
from jax import lax
from jax.experimental import pallas as pl
from jax.experimental.pallas import tpu as pltpu
from jax.sharding import PartitionSpec as P

MESH = pl.DeviceIdType.MESH
F32, BF16, I32 = jnp.float32, jnp.bfloat16, jnp.int32
SIDE = 8
NODES = SIDE**3
ROWS = NODES // 128
PAIR = 256
BATCH = 32


def blocks_along(span):
    edge = round((span // NODES) ** (1 / 3))
    assert edge**3 * NODES == span and 1 < edge <= 3
    return edge


def iota(shape, axis):
    return lax.broadcasted_iota(I32, shape, axis)


def halves(x):
    high = x.astype(BF16)
    low = (x - high.astype(F32)).astype(BF16)
    return jnp.concatenate([high, low], axis=0)


def add_rows(index_ref, value_ref, table_ref):
    def step(b, carry):
        base = pl.multiple_of(b * BATCH, BATCH)
        nodes = [index_ref[base + k] for k in range(BATCH)]
        held = [table_ref[pl.ds(n, 1), :] for n in nodes]
        sums = [held[k] + value_ref[pl.ds(base + k, 1), :] for k in range(BATCH)]
        for k in range(BATCH):
            table_ref[pl.ds(nodes[k], 1), :] = sums[k]
        return carry

    lax.fori_loop(0, index_ref.shape[0] // BATCH, step, 0)


def take_rows(index_ref, table_ref, out_ref):
    def step(b, carry):
        base = pl.multiple_of(b * BATCH, BATCH)
        rows = [table_ref[pl.ds(index_ref[base + k], 1), :] for k in range(BATCH)]
        for k in range(BATCH):
            out_ref[pl.ds(base + k, 1), :] = rows[k]
        return carry

    lax.fori_loop(0, index_ref.shape[0] // BATCH, step, 0)


def to_rows(flat_ref, rows_ref):
    def step(t, carry):
        base = pl.multiple_of(t * 128, 128)
        block = flat_ref[:, pl.ds(base, 128)]
        wide = jnp.concatenate([block] * (128 // block.shape[0]), axis=0)
        rows_ref[pl.ds(base, 128), :] = wide.T
        return carry

    lax.fori_loop(0, flat_ref.shape[1] // 128, step, 0)


def from_rows(rows_ref, flat_ref, put):
    def step(t, carry):
        base = pl.multiple_of(t * 128, 128)
        put(base, rows_ref[pl.ds(base, 128), :].T[: flat_ref.shape[0]])
        return carry

    lax.fori_loop(0, flat_ref.shape[1] // 128, step, 0)


def general_table(map_hbm, value_ref, map_smem, rows_ref, table_ref):
    pltpu.sync_copy(map_hbm, map_smem)
    chunk = 96

    def clear(b, carry):
        base = pl.multiple_of(b * chunk, chunk)
        table_ref[pl.ds(base, chunk), :] = jnp.zeros((chunk, 128), F32)
        return carry

    lax.fori_loop(0, table_ref.shape[0] // chunk, clear, 0)
    to_rows(value_ref, rows_ref)
    add_rows(map_smem, rows_ref, table_ref)


def sweep(ref, edge, base=None, out=None):
    lane = iota((ref.shape[0], 128), 1)
    zero = jnp.zeros((ref.shape[0], 128), F32)

    def at(px, py, pz, row):
        return pl.ds((((px * edge + py) * edge + pz) * ROWS + row) * 128, 128)

    def line(spots_of, first, last, shift, final=False):
        held = [ref[:, s] for s in spots_of]
        for i, s in enumerate(spots_of):
            total = held[i]
            if i + 1 < edge:
                total = total + jnp.where(last, pltpu.roll(held[i + 1], shift, 1), zero)
            if i > 0:
                total = total + jnp.where(first, pltpu.roll(held[i - 1], 128 - shift, 1), zero)
            if final and base is not None:
                out[:, s] = total + base[:, s]
            else:
                ref[:, s] = total

    for py in range(edge):
        for pz in range(edge):
            for px in range(edge - 1):
                a, b = at(px, py, pz, ROWS - 1), at(px + 1, py, pz, 0)
                upper, lower = ref[:, a], ref[:, b]
                ref[:, a] = upper + jnp.where(lane >= 64, pltpu.roll(lower, 64, 1), zero)
                ref[:, b] = lower + jnp.where(lane < 64, pltpu.roll(upper, 64, 1), zero)
    y, z = (lane // SIDE) % SIDE, lane % SIDE
    for px in range(edge):
        for pz in range(edge):
            for row in range(ROWS):
                line([at(px, py, pz, row) for py in range(edge)], y == 0, y == SIDE - 1, SIDE * (SIDE - 1))
        for py in range(edge):
            for row in range(ROWS):
                line([at(px, py, pz, row) for pz in range(edge)], z == 0, z == SIDE - 1, SIDE - 1, True)


def find_places(lab_ref, edge):
    count = edge**3
    near, mid, far = (lab_ref[pl.ds(k, 32, stride=ROWS), :].astype(F32) for k in (0, 1, ROWS - 1))
    near_t, mid_t, far_t = near.T, mid.T, far.T
    real = (iota((32, 32), 0) < count) & (iota((32, 32), 1) < count)
    sides = (
        (near, near_t, 27, far, far_t, 91),
        (mid, mid_t, 67, mid, mid_t, 123),
        (mid, mid_t, 88, mid, mid_t, 95),
    )
    place = jnp.zeros((32, 1), F32)
    for low, low_t, i, high, high_t, j in sides:
        before = jnp.where(real & (low[:, i : i + 1] == high_t[j : j + 1, :]), 1.0, 0.0)
        before_t = jnp.where(real & (high[:, j : j + 1] == low_t[i : i + 1, :]), 1.0, 0.0)
        steps = jnp.zeros((1, 32), F32)
        if edge > 2:
            steps = jnp.sum(before_t, axis=0, keepdims=True)
        place = place * edge + jnp.sum(before * (1.0 + steps), axis=1, keepdims=True)
    hit = (iota((32, 32), 0) < count) & (place == iota((32, 32), 1).astype(F32))
    who = jnp.sum(jnp.where(hit, iota((32, 32), 0).astype(F32), 0.0), axis=0, keepdims=True)
    times = jnp.sum(jnp.where(hit, 1.0, 0.0), axis=0, keepdims=True)
    wrong = jnp.where((iota((1, 32), 1) < count) & (times != 1.0), 1, 0)
    return jnp.clip(who.astype(I32), 0, count - 1), wrong


def count_mismatches(grid_ref, edge):
    total = jnp.zeros((1, 128), I32)
    lane = iota((1, 128), 1)
    y, z = (lane // SIDE) % SIDE, lane % SIDE
    for axis, stride in enumerate((edge * edge, edge, 1)):
        rows = (edge**3 - stride) * ROWS
        start = stride * ROWS - (ROWS - 1 if axis == 0 else 0)
        inner = (iota((rows, 1), 0) // ROWS // stride) % edge < edge - 1
        if axis == 0:
            where, shift = inner & (iota((rows, 1), 0) % ROWS == ROWS - 1) & (lane < 64), 64
        elif axis == 1:
            where, shift = inner & (y == 0), 128 - SIDE * (SIDE - 1)
        else:
            where, shift = inner & (z == 0), 128 - (SIDE - 1)
        low, high = grid_ref[0:rows, :], grid_ref[start : start + rows, :]
        differ = where & (pltpu.roll(low, shift, 1) != high)
        total = total + jnp.sum(jnp.where(differ, 1, 0), axis=0, keepdims=True)
    return total


def order_kernel(
    edge, slot_count, map_hbm, node_hbm, count_hbm, value_hbm, map_flat, node_flat,
    order_ref, node_ref, flag_ref, picked_ref, grid_ref,
    lab_ref, raw_ref, count_ref, sems, value_ref, map_smem, node_smem, rows_ref, table_ref,
):
    count = edge**3
    lines = order_ref.shape[0]
    slot_rows = node_ref.shape[0]
    labels = pltpu.make_async_copy(map_hbm, lab_ref.at[0:lines, :], sems.at[0])
    nodes = pltpu.make_async_copy(node_hbm, raw_ref, sems.at[1])
    counts = pltpu.make_async_copy(count_hbm, count_ref, sems.at[2])
    values = pltpu.make_async_copy(value_hbm, value_ref, sems.at[3])
    for copy in (labels, nodes, counts, values):
        copy.start()
    lab_ref[lines:, :] = jnp.zeros((lab_ref.shape[0] - lines, 128), I32)
    labels.wait()
    who, wrong = find_places(lab_ref, edge)
    flag_ref[...] = jnp.zeros((8, 128), I32)
    flag_ref[0:1, 0:32] = who
    values.wait()
    for s in range(count):
        e = who[0, s]
        grid_ref[:, s * NODES : (s + 1) * NODES] = value_ref[:, pl.ds(pl.multiple_of(e * NODES, NODES), NODES)]
        for r in range(ROWS):
            order_ref[s * ROWS + r : s * ROWS + r + 1, :] = lab_ref[pl.ds(e * ROWS + r, 1), :]
    nodes.wait()
    counts.wait()
    per = slot_count // 128
    row_of = iota((slot_rows, 128), 0)
    limit = jnp.zeros((slot_rows, 128), I32)
    for p in range(slot_rows // per):
        limit = jnp.where(row_of // per == p, count_ref[p], limit)
    live = (row_of % per) * 128 + iota((slot_rows, 128), 1) < limit
    node_ref[...] = jnp.where(live, raw_ref[...], -1)
    bad = jnp.sum(count_mismatches(order_ref, edge)) + jnp.sum(wrong)
    flag_ref[1:2, :] = jnp.full((1, 128), bad, I32)

    @pl.when(bad > 0)
    def _():
        general_table(map_flat, value_ref, map_smem, rows_ref, table_ref)
        pltpu.sync_copy(node_flat, node_smem)
        take_rows(node_smem, table_ref, rows_ref)

        def put(base, block):
            p = base // slot_count
            keep = base - p * slot_count + iota((8, 128), 1) < count_ref[p]
            picked_ref[:, pl.ds(base, 128)] = jnp.where(keep, block, 0.0)

        from_rows(rows_ref, picked_ref, put)


def finish_kernel(
    edge, slot_count, delta_in, grid_ref, flag_ref, change_ref, count_hbm, value_hbm, map_flat, node_flat,
    out_hbm,
    delta_ref, flags, count_ref, sems, map_smem, node_smem, rows_ref, table_ref,
):
    count = edge**3
    slots_all = change_ref.shape[1]
    marks = pltpu.make_async_copy(flag_ref, flags, sems.at[0])
    marks.start()
    sweep(delta_in, edge, grid_ref, delta_ref)
    marks.wait()
    for s in range(count):
        spot = pl.ds(pl.multiple_of(flags[0, s] * NODES, NODES), NODES)
        pltpu.make_async_copy(delta_ref.at[:, s * NODES : (s + 1) * NODES], out_hbm.at[:, spot], sems.at[1]).start()
    pltpu.make_async_copy(delta_ref, out_hbm, sems.at[1]).wait()

    @pl.when(flags[1, 0] > 0)
    def _():
        pltpu.sync_copy(value_hbm, delta_ref)
        pltpu.sync_copy(count_hbm, count_ref)
        general_table(map_flat, delta_ref, map_smem, rows_ref, table_ref)
        pltpu.sync_copy(node_flat, node_smem)
        to_rows(change_ref, rows_ref)
        spare = table_ref.shape[0] - 1

        def bury(i, carry):
            p = i // slot_count
            node_smem[i] = jnp.where(i - p * slot_count < count_ref[p], node_smem[i], spare)
            return carry

        lax.fori_loop(0, slots_all, bury, 0)
        add_rows(node_smem, rows_ref, table_ref)
        take_rows(map_smem, table_ref, rows_ref)

        def put(base, block):
            delta_ref[:, pl.ds(base, 128)] = block

        from_rows(rows_ref, delta_ref, put)
        pltpu.sync_copy(delta_ref, out_hbm)


def find_nodes(edge, order_ref, a_ref, b_ref):
    lines = order_ref.shape[0]
    tall16 = a_ref.shape[0] // 2
    lane = iota((1, 128), 1)
    first = (lane >= 64, (lane // SIDE) % SIDE > 0, lane % SIDE > 0)
    high_of = iota((tall16, 128), 0).astype(BF16)
    low_of = iota((128, 128), 0).astype(BF16)
    zero = jnp.bfloat16(0)
    for r in range(lines):
        s = r // ROWS
        place = (s // (edge * edge), (s // edge) % edge, s % edge)
        label = order_ref[r : r + 1, :]
        for axis in range(3):
            if place[axis] > 0 and (axis > 0 or r % ROWS == 0):
                label = jnp.where(first[axis], label, -1)
        high = jnp.broadcast_to((label >> 7).astype(BF16), (tall16, 128))
        low = jnp.broadcast_to((label & 127).astype(BF16), (128, 128))
        col = slice(r * 128, (r + 1) * 128)
        within = jnp.broadcast_to((lane + (r % 2) * 128).astype(BF16), (tall16, 128))
        hit = high == high_of
        a_ref[0:tall16, col] = jnp.where(hit, jnp.bfloat16(r // 2), zero)
        a_ref[tall16:, col] = jnp.where(hit, within, zero)
        b_ref[:, col] = jnp.where(low == low_of, jnp.bfloat16(1), zero)
    found = lax.dot_general(a_ref[...], b_ref[...], (((1,), (1,)), ((), ())), preferred_element_type=F32)
    return found[0:tall16] * PAIR + found[tall16:]


def exchange_kernel(
    groups, places, edge, order_ref, node_ref, owned_ref, flag_ref, other_ref, raw_ref,
    grid_ref, delta_ref, change_ref,
    picked, inbox, reply, back, spot_ref, pa_ref, pb_ref, u_ref, tb_ref, sb_ref,
    send_out, recv_out, send_back, recv_back,
):
    fields, slots_all = change_ref.shape
    size = slots_all // (3 * places)
    heads = 2 * size // 128
    blocks = grid_ref.shape[1] // PAIR
    g, l = lax.axis_index("grp"), lax.axis_index("loc")

    far = [jnp.where(m > l, m - l, l - m) for m in range(places)]
    rank = [
        sum(((far[n] > far[m]) | ((far[n] == far[m]) & (n > m))).astype(I32) for n in range(places) if n != m)
        for m in range(places)
    ]
    places_by = [sum(jnp.where(rank[m] == i, m, 0) for m in range(places)) for i in range(places - 1)] + [l]

    def group(k):
        return lax.rem(g + groups + k, groups)

    def others(i):
        return (0, 2) if i == places - 1 else (0, 2, 1)

    def part(k, place):
        return pl.ds(pl.multiple_of((k * places + place) * size, 128), size)

    def lines_of(k, place):
        return [pl.ds((k * places + place) * (size // 128) + j, 1) for j in range(size // 128)]

    def copy(k, src, dst, there, near, sems, device):
        return pltpu.make_async_remote_copy(
            src_ref=src.at[:, part(k, there)],
            dst_ref=dst.at[:, part(k, near)],
            send_sem=sems[0].at[k * places + there],
            recv_sem=sems[1].at[k * places + near],
            device_id=device,
            device_id_type=MESH,
        )

    def outward(k, m):
        return copy(k, picked, inbox, m, l, (send_out, recv_out), (group(k - 1), m))

    def inward(k, m):
        return copy(k, picked, inbox, m, m, (send_out, recv_out), (group(1 - k), m))

    def homeward(k, m):
        return copy(k, reply, back, m, l, (send_back, recv_back), (group(1 - k), m))

    def returned(k, m):
        return copy(k, reply, back, m, m, (send_back, recv_back), (group(k - 1), m))

    barrier = pltpu.get_barrier_semaphore()
    for i in range(places):
        for k in others(i):
            pl.semaphore_signal(barrier, inc=1, device_id=(group(k - 1), places_by[i]), device_id_type=MESH)

    zero = jnp.bfloat16(0)
    where_is = find_nodes(edge, order_ref, pa_ref, pb_ref)
    grid_ref[...] = raw_ref[...]
    sweep(grid_ref, edge)
    for r in range(blocks):
        u_ref[r * 16 : (r + 1) * 16, :] = halves(grid_ref[:, r * PAIR : (r + 1) * PAIR])

    def spots_of(k, i):
        row = i * (spot_ref.shape[0] // places) + k * (size // 128)
        return jnp.concatenate([spot_ref[row + j : row + j + 1, :] for j in range(size // 128)], axis=1)

    def owned_of(k, m):
        return jnp.concatenate([owned_ref[line, :] for line in lines_of(k, m)], axis=1)

    def onehot(index, count):
        low = jnp.broadcast_to((index & (count - 1)).astype(BF16), (count, size))
        return jnp.where(low == iota((count, size), 0).astype(BF16), jnp.bfloat16(1), zero)

    tall = (((SIDE - 1) * edge + 1) ** 3 + 127) // 128

    def look_up(i, m):
        rows = [line for k in range(3) for line in lines_of(k, m)]
        spare = [jnp.full((8 - len(rows) % 8, 128), -1, I32)] if len(rows) % 8 else []
        node = jnp.concatenate([node_ref[line, :] for line in rows] + spare, axis=0)
        high, low = node >> 7, node & 127
        spot = jnp.full(node.shape, -float(PAIR), F32)
        for h in range(tall):
            row = jnp.broadcast_to(where_is[h : h + 1, :], node.shape)
            spot = jnp.where(high == h, jnp.take_along_axis(row, low, axis=1), spot)
        spot_ref[i * spot.shape[0] : (i + 1) * spot.shape[0], :] = spot.astype(I32)

    def pick_by_lane(spots):
        parts = []
        for j in range(size // 128):
            index = jnp.broadcast_to(spots[:, j * 128 : (j + 1) * 128], (fields, 128))
            which, low = index >> 7, index & 127
            value = jnp.zeros((fields, 128), F32)
            for r in range(2 * blocks):
                held = jnp.take_along_axis(grid_ref[:, r * 128 : (r + 1) * 128], low, axis=1)
                value = jnp.where(which == r, held, value)
            parts.append(value)
        return jnp.concatenate(parts, axis=1)

    general = jnp.concatenate([flag_ref[1:2, :]] * (size // 128), axis=1) > 0
    for i in range(places):
        m = places_by[i]
        look_up(i, m)
        by_lane = pick_by_lane(spots_of(1, i))
        picked[:, part(1, m)] = jnp.where(general, other_ref[:, part(1, m)], by_lane)
        for k in (0, 2):
            spots = spots_of(k, i)
            both = jnp.dot(u_ref[...], onehot(spots, PAIR), preferred_element_type=F32)
            which = jnp.broadcast_to(spots >> 8, (fields, size))
            top = jnp.zeros((fields, size), F32)
            rest = jnp.zeros((fields, size), F32)
            for r in range(blocks):
                mine = which == r
                top = jnp.where(mine, both[r * 16 : r * 16 + 8], top)
                rest = jnp.where(mine, both[r * 16 + 8 : r * 16 + 16], rest)
            picked[:, part(k, m)] = jnp.where(general, other_ref[:, part(k, m)], top + rest)
        if i == 1:
            pl.semaphore_wait(barrier, 3 * places - 1)
        for n in range(0 if i == 1 else i, i + 1 if i else 0):
            for k in others(n):
                outward(k, places_by[n]).start()

    for i in range(places):
        for k in range(3):
            column = ((places - 1 - i) * 3 + k) * size
            sb_ref[:, column : column + size] = onehot(spots_of(k, i), PAIR)
            tb_ref[:, part(k, places_by[i])] = onehot(owned_of(k, places_by[i]), 128)
    summed = jnp.zeros((heads * 16, 128), F32)
    for i in reversed(range(places)):
        m = places_by[i]
        for k in others(i):
            inward(k, m).wait_recv()
        lefts = []
        for k in range(3):
            source = picked if (i, k) == (places - 1, 1) else inbox
            both = halves(source[:, part(k, m)])
            which = jnp.broadcast_to((owned_of(k, m) >> 7).astype(BF16), (16, size))
            lefts.append(jnp.concatenate([jnp.where(which == jnp.bfloat16(h), both, zero) for h in range(heads)], axis=0))
        right = jnp.concatenate([tb_ref[:, part(k, m)] for k in range(3)], axis=1)
        summed = summed + lax.dot_general(
            jnp.concatenate(lefts, axis=1), right, (((1,), (1,)), ((), ())), preferred_element_type=F32
        )
    totals = [summed[h * 16 : h * 16 + 8] + summed[h * 16 + 8 : h * 16 + 16] for h in range(heads)]
    for i in range(places):
        m = places_by[i]
        for k in range(3):
            owned = owned_of(k, m)
            for j in range(size // 128):
                index = jnp.broadcast_to(owned[:, j * 128 : (j + 1) * 128], (fields, 128))
                low, which = index & 127, index >> 7
                total = jnp.zeros((fields, 128), F32)
                for h in range(heads):
                    total = jnp.where(which == h, jnp.take_along_axis(totals[h], low, axis=1), total)
                reply[:, pl.ds(pl.multiple_of((k * places + m) * size + j * 128, 128), 128)] = total
        for k in others(i):
            homeward(k, m).start()

    order = [i for i in reversed(range(places))]
    for first, last in tuple((n, n + 1) for n in range(places)):
        together = order[first:last]
        lefts = []
        for i in together:
            m = places_by[i]
            for k in others(i):
                returned(k, m).wait_recv()
            for k in range(3):
                source = reply if (i, k) == (places - 1, 1) else back
                change = source[:, part(k, m)] - picked[:, part(k, m)]
                change_ref[:, part(k, m)] = change
                both = halves(change)
                which = jnp.broadcast_to((spots_of(k, i) >> 8).astype(BF16), (16, size))
                lefts.append(jnp.concatenate([jnp.where(which == jnp.bfloat16(r), both, zero) for r in range(blocks)], axis=0))
        depth = len(together) * 3 * size
        start = first * 3 * size
        spread = lax.dot_general(
            jnp.concatenate(lefts, axis=1), sb_ref[:, start : start + depth], (((1,), (1,)), ((), ())), preferred_element_type=F32
        )
        for r in range(blocks):
            col = slice(r * PAIR, (r + 1) * PAIR)
            moved = spread[r * 16 : r * 16 + 8] + spread[r * 16 + 8 : r * 16 + 16]
            if first == 0:
                delta_ref[:, col] = moved
            else:
                delta_ref[:, col] += moved

    for i in range(places):
        for k in others(i):
            outward(k, places_by[i]).wait_send()
            homeward(k, places_by[i]).wait_send()


SMEM = pl.BlockSpec(memory_space=pltpu.SMEM)
VMEM = pl.BlockSpec(memory_space=pltpu.VMEM)
HBM = pl.BlockSpec(memory_space=pltpu.HBM)


def on_device(groups, places, element_values, local_map, send_node, send_count, recv_slot):
    fields, span = element_values.shape
    slots_all = send_node.shape[1]
    slot_count = slots_all // (3 * places)
    edge = blocks_along(span)
    local = ((SIDE - 1) * edge + 1) ** 3
    tall16 = (local + 2047) // 2048 * 16
    table = (local + 96) // 96 * 96
    lines, slot_rows = span // 128, slots_all // 128
    map_rows, node_rows = local_map.reshape(-1, 128), send_node.reshape(-1, 128)
    owned_rows = recv_slot.reshape(-1, 128)
    element_values, local_map, map_rows, node_rows, nodes, counts = (
        pltpu.with_memory_space_constraint(x, pltpu.HBM)
        for x in (element_values, local_map, map_rows, node_rows, send_node.reshape(-1), send_count.reshape(-1))
    )
    shape = jax.ShapeDtypeStruct
    general = [
        pltpu.SMEM((span,), I32),
        pltpu.SMEM((slots_all,), I32),
        pltpu.VMEM((span, 128), F32),
        pltpu.VMEM((table, 128), F32),
    ]
    order, live_nodes, flags, other, raw = pl.pallas_call(
        functools.partial(order_kernel, edge, slot_count),
        out_shape=(
            shape((lines, 128), I32),
            shape((slot_rows, 128), I32),
            shape((8, 128), I32),
            shape((fields, slots_all), F32),
            shape((fields, span), F32),
        ),
        in_specs=[HBM] * 6,
        out_specs=(VMEM,) * 5,
        scratch_shapes=[
            pltpu.VMEM((32 * ROWS, 128), I32),
            pltpu.VMEM((slot_rows, 128), I32),
            pltpu.SMEM(counts.shape, I32),
            pltpu.SemaphoreType.DMA((4,)),
            pltpu.VMEM((fields, span), F32),
        ]
        + general,
        compiler_params=pltpu.CompilerParams(vmem_limit_bytes=24 * 1024 * 1024),
    )(map_rows, node_rows, counts, element_values, local_map, nodes)
    grid, delta, change = pl.pallas_call(
        functools.partial(exchange_kernel, groups, places, edge),
        out_shape=(shape((fields, span), F32), shape((fields, span), F32), shape((fields, slots_all), F32)),
        in_specs=[VMEM] * 6,
        out_specs=(VMEM,) * 3,
        scratch_shapes=[pltpu.VMEM((fields, slots_all), F32)] * 4
        + [
            pltpu.VMEM((places * ((3 * slot_count // 128 + 7) // 8 * 8), 128), I32),
            pltpu.VMEM((2 * tall16, span), BF16),
            pltpu.VMEM((128, span), BF16),
            pltpu.VMEM((lines // 2 * 16, PAIR), BF16),
            pltpu.VMEM((128, slots_all), BF16),
            pltpu.VMEM((PAIR, slots_all), BF16),
        ]
        + [pltpu.SemaphoreType.DMA((3 * places,))] * 4,
        compiler_params=pltpu.CompilerParams(
            collective_id=0, has_side_effects=True, vmem_limit_bytes=40 * 1024 * 1024
        ),
    )(order, live_nodes, owned_rows, flags, other, raw)
    return pl.pallas_call(
        functools.partial(finish_kernel, edge, slot_count),
        out_shape=shape((fields, span), F32),
        in_specs=[VMEM] * 4 + [HBM] * 4,
        out_specs=HBM,
        scratch_shapes=[
            pltpu.VMEM((fields, span), F32),
            pltpu.SMEM((8, 128), I32),
            pltpu.SMEM(counts.shape, I32),
            pltpu.SemaphoreType.DMA((2,)),
        ]
        + general,
        compiler_params=pltpu.CompilerParams(vmem_limit_bytes=24 * 1024 * 1024),
    )(delta, grid, flags, change, counts, element_values, local_map, nodes)


def solution(mesh):
    return jax.shard_map(
        functools.partial(on_device, mesh.shape["grp"], mesh.shape["loc"]),
        mesh=mesh,
        in_specs=(
            P(None, ("grp", "loc")),
            P(("grp", "loc")),
            P(("grp", "loc"), None),
            P(("grp", "loc"), None),
            P(("grp", "loc"), None),
        ),
        out_specs=P(None, ("grp", "loc")),
        check_vma=False,
    )
```

```python
import functools

import jax
import jax.numpy as jnp
from jax import lax
from jax.experimental import pallas as pl
from jax.experimental.pallas import tpu as pltpu
from jax.sharding import PartitionSpec as P

MESH = pl.DeviceIdType.MESH
F32, BF16, I32 = jnp.float32, jnp.bfloat16, jnp.int32
SIDE = 8
NODES = SIDE**3
ROWS = NODES // 128
PAIR = 256
BATCH = 32


def blocks_along(span):
    edge = round((span // NODES) ** (1 / 3))
    assert edge**3 * NODES == span and 1 < edge <= 3
    return edge


def iota(shape, axis):
    return lax.broadcasted_iota(I32, shape, axis)


def halves(x):
    high = x.astype(BF16)
    low = (x - high.astype(F32)).astype(BF16)
    return jnp.concatenate([high, low], axis=0)


def add_rows(index_ref, value_ref, table_ref):
    def step(b, carry):
        base = pl.multiple_of(b * BATCH, BATCH)
        nodes = [index_ref[base + k] for k in range(BATCH)]
        held = [table_ref[pl.ds(n, 1), :] for n in nodes]
        sums = [held[k] + value_ref[pl.ds(base + k, 1), :] for k in range(BATCH)]
        for k in range(BATCH):
            table_ref[pl.ds(nodes[k], 1), :] = sums[k]
        return carry

    lax.fori_loop(0, index_ref.shape[0] // BATCH, step, 0)


def take_rows(index_ref, table_ref, out_ref):
    def step(b, carry):
        base = pl.multiple_of(b * BATCH, BATCH)
        rows = [table_ref[pl.ds(index_ref[base + k], 1), :] for k in range(BATCH)]
        for k in range(BATCH):
            out_ref[pl.ds(base + k, 1), :] = rows[k]
        return carry

    lax.fori_loop(0, index_ref.shape[0] // BATCH, step, 0)


def to_rows(flat_ref, rows_ref):
    def step(t, carry):
        base = pl.multiple_of(t * 128, 128)
        block = flat_ref[:, pl.ds(base, 128)]
        wide = jnp.concatenate([block] * (128 // block.shape[0]), axis=0)
        rows_ref[pl.ds(base, 128), :] = wide.T
        return carry

    lax.fori_loop(0, flat_ref.shape[1] // 128, step, 0)


def from_rows(rows_ref, flat_ref, put):
    def step(t, carry):
        base = pl.multiple_of(t * 128, 128)
        put(base, rows_ref[pl.ds(base, 128), :].T[: flat_ref.shape[0]])
        return carry

    lax.fori_loop(0, flat_ref.shape[1] // 128, step, 0)


def general_table(map_hbm, value_ref, map_smem, rows_ref, table_ref):
    pltpu.sync_copy(map_hbm, map_smem)
    chunk = 96

    def clear(b, carry):
        base = pl.multiple_of(b * chunk, chunk)
        table_ref[pl.ds(base, chunk), :] = jnp.zeros((chunk, 128), F32)
        return carry

    lax.fori_loop(0, table_ref.shape[0] // chunk, clear, 0)
    to_rows(value_ref, rows_ref)
    add_rows(map_smem, rows_ref, table_ref)


def sweep(ref, edge, base=None, out=None):
    lane = iota((ref.shape[0], 128), 1)
    zero = jnp.zeros((ref.shape[0], 128), F32)

    def at(px, py, pz, row):
        return pl.ds((((px * edge + py) * edge + pz) * ROWS + row) * 128, 128)

    def line(spots_of, first, last, shift, final=False):
        held = [ref[:, s] for s in spots_of]
        for i, s in enumerate(spots_of):
            total = held[i]
            if i + 1 < edge:
                total = total + jnp.where(last, pltpu.roll(held[i + 1], shift, 1), zero)
            if i > 0:
                total = total + jnp.where(first, pltpu.roll(held[i - 1], 128 - shift, 1), zero)
            if final and base is not None:
                out[:, s] = total + base[:, s]
            else:
                ref[:, s] = total

    for py in range(edge):
        for pz in range(edge):
            for px in range(edge - 1):
                a, b = at(px, py, pz, ROWS - 1), at(px + 1, py, pz, 0)
                upper, lower = ref[:, a], ref[:, b]
                ref[:, a] = upper + jnp.where(lane >= 64, pltpu.roll(lower, 64, 1), zero)
                ref[:, b] = lower + jnp.where(lane < 64, pltpu.roll(upper, 64, 1), zero)
    y, z = (lane // SIDE) % SIDE, lane % SIDE
    for px in range(edge):
        for pz in range(edge):
            for row in range(ROWS):
                line([at(px, py, pz, row) for py in range(edge)], y == 0, y == SIDE - 1, SIDE * (SIDE - 1))
        for py in range(edge):
            for row in range(ROWS):
                line([at(px, py, pz, row) for pz in range(edge)], z == 0, z == SIDE - 1, SIDE - 1, True)


def find_places(lab_ref, edge):
    count = edge**3
    near, mid, far = (lab_ref[pl.ds(k, 32, stride=ROWS), :].astype(F32) for k in (0, 1, ROWS - 1))
    near_t, mid_t, far_t = near.T, mid.T, far.T
    real = (iota((32, 32), 0) < count) & (iota((32, 32), 1) < count)
    sides = (
        (near, near_t, 27, far, far_t, 91),
        (mid, mid_t, 67, mid, mid_t, 123),
        (mid, mid_t, 88, mid, mid_t, 95),
    )
    place = jnp.zeros((32, 1), F32)
    for low, low_t, i, high, high_t, j in sides:
        before = jnp.where(real & (low[:, i : i + 1] == high_t[j : j + 1, :]), 1.0, 0.0)
        before_t = jnp.where(real & (high[:, j : j + 1] == low_t[i : i + 1, :]), 1.0, 0.0)
        steps = jnp.zeros((1, 32), F32)
        if edge > 2:
            steps = jnp.sum(before_t, axis=0, keepdims=True)
        place = place * edge + jnp.sum(before * (1.0 + steps), axis=1, keepdims=True)
    hit = (iota((32, 32), 0) < count) & (place == iota((32, 32), 1).astype(F32))
    who = jnp.sum(jnp.where(hit, iota((32, 32), 0).astype(F32), 0.0), axis=0, keepdims=True)
    times = jnp.sum(jnp.where(hit, 1.0, 0.0), axis=0, keepdims=True)
    wrong = jnp.where((iota((1, 32), 1) < count) & (times != 1.0), 1, 0)
    return jnp.clip(who.astype(I32), 0, count - 1), wrong


def count_mismatches(grid_ref, edge):
    total = jnp.zeros((1, 128), I32)
    lane = iota((1, 128), 1)
    y, z = (lane // SIDE) % SIDE, lane % SIDE
    for axis, stride in enumerate((edge * edge, edge, 1)):
        rows = (edge**3 - stride) * ROWS
        start = stride * ROWS - (ROWS - 1 if axis == 0 else 0)
        inner = (iota((rows, 1), 0) // ROWS // stride) % edge < edge - 1
        if axis == 0:
            where, shift = inner & (iota((rows, 1), 0) % ROWS == ROWS - 1) & (lane < 64), 64
        elif axis == 1:
            where, shift = inner & (y == 0), 128 - SIDE * (SIDE - 1)
        else:
            where, shift = inner & (z == 0), 128 - (SIDE - 1)
        low, high = grid_ref[0:rows, :], grid_ref[start : start + rows, :]
        differ = where & (pltpu.roll(low, shift, 1) != high)
        total = total + jnp.sum(jnp.where(differ, 1, 0), axis=0, keepdims=True)
    return total


def order_kernel(
    edge, slot_count, map_hbm, node_hbm, count_hbm, value_hbm, map_flat, node_flat,
    order_ref, node_ref, flag_ref, picked_ref, grid_ref,
    lab_ref, raw_ref, count_ref, sems, value_ref, map_smem, node_smem, rows_ref, table_ref,
):
    count = edge**3
    lines = order_ref.shape[0]
    slot_rows = node_ref.shape[0]
    labels = pltpu.make_async_copy(map_hbm, lab_ref.at[0:lines, :], sems.at[0])
    nodes = pltpu.make_async_copy(node_hbm, raw_ref, sems.at[1])
    counts = pltpu.make_async_copy(count_hbm, count_ref, sems.at[2])
    values = pltpu.make_async_copy(value_hbm, value_ref, sems.at[3])
    for copy in (labels, nodes, counts, values):
        copy.start()
    lab_ref[lines:, :] = jnp.zeros((lab_ref.shape[0] - lines, 128), I32)
    labels.wait()
    who, wrong = find_places(lab_ref, edge)
    flag_ref[...] = jnp.zeros((8, 128), I32)
    flag_ref[0:1, 0:32] = who
    values.wait()
    for s in range(count):
        e = who[0, s]
        grid_ref[:, s * NODES : (s + 1) * NODES] = value_ref[:, pl.ds(pl.multiple_of(e * NODES, NODES), NODES)]
        for r in range(ROWS):
            order_ref[s * ROWS + r : s * ROWS + r + 1, :] = lab_ref[pl.ds(e * ROWS + r, 1), :]
    nodes.wait()
    counts.wait()
    per = slot_count // 128
    row_of = iota((slot_rows, 128), 0)
    limit = jnp.zeros((slot_rows, 128), I32)
    for p in range(slot_rows // per):
        limit = jnp.where(row_of // per == p, count_ref[p], limit)
    live = (row_of % per) * 128 + iota((slot_rows, 128), 1) < limit
    node_ref[...] = jnp.where(live, raw_ref[...], -1)
    bad = jnp.sum(count_mismatches(order_ref, edge)) + jnp.sum(wrong)
    flag_ref[1:2, :] = jnp.full((1, 128), bad, I32)

    @pl.when(bad > 0)
    def _():
        general_table(map_flat, value_ref, map_smem, rows_ref, table_ref)
        pltpu.sync_copy(node_flat, node_smem)
        take_rows(node_smem, table_ref, rows_ref)

        def put(base, block):
            p = base // slot_count
            keep = base - p * slot_count + iota((8, 128), 1) < count_ref[p]
            picked_ref[:, pl.ds(base, 128)] = jnp.where(keep, block, 0.0)

        from_rows(rows_ref, picked_ref, put)


def finish_kernel(
    edge, slot_count, delta_in, grid_ref, flag_ref, change_ref, count_hbm, value_hbm, map_flat, node_flat,
    out_hbm,
    delta_ref, flags, count_ref, sems, map_smem, node_smem, rows_ref, table_ref,
):
    count = edge**3
    slots_all = change_ref.shape[1]
    marks = pltpu.make_async_copy(flag_ref, flags, sems.at[0])
    marks.start()
    sweep(delta_in, edge, grid_ref, delta_ref)
    marks.wait()
    for s in range(count):
        spot = pl.ds(pl.multiple_of(flags[0, s] * NODES, NODES), NODES)
        pltpu.make_async_copy(delta_ref.at[:, s * NODES : (s + 1) * NODES], out_hbm.at[:, spot], sems.at[1]).start()
    pltpu.make_async_copy(delta_ref, out_hbm, sems.at[1]).wait()

    @pl.when(flags[1, 0] > 0)
    def _():
        pltpu.sync_copy(value_hbm, delta_ref)
        pltpu.sync_copy(count_hbm, count_ref)
        general_table(map_flat, delta_ref, map_smem, rows_ref, table_ref)
        pltpu.sync_copy(node_flat, node_smem)
        to_rows(change_ref, rows_ref)
        spare = table_ref.shape[0] - 1

        def bury(i, carry):
            p = i // slot_count
            node_smem[i] = jnp.where(i - p * slot_count < count_ref[p], node_smem[i], spare)
            return carry

        lax.fori_loop(0, slots_all, bury, 0)
        add_rows(node_smem, rows_ref, table_ref)
        take_rows(map_smem, table_ref, rows_ref)

        def put(base, block):
            delta_ref[:, pl.ds(base, 128)] = block

        from_rows(rows_ref, delta_ref, put)
        pltpu.sync_copy(delta_ref, out_hbm)


def find_nodes(edge, order_ref, a_ref, b_ref):
    lines = order_ref.shape[0]
    tall16 = a_ref.shape[0] // 2
    lane = iota((1, 128), 1)
    first = (lane >= 64, (lane // SIDE) % SIDE > 0, lane % SIDE > 0)
    high_of = iota((tall16, 128), 0).astype(BF16)
    low_of = iota((128, 128), 0).astype(BF16)
    zero = jnp.bfloat16(0)
    for r in range(lines):
        s = r // ROWS
        place = (s // (edge * edge), (s // edge) % edge, s % edge)
        label = order_ref[r : r + 1, :]
        for axis in range(3):
            if place[axis] > 0 and (axis > 0 or r % ROWS == 0):
                label = jnp.where(first[axis], label, -1)
        high = jnp.broadcast_to((label >> 7).astype(BF16), (tall16, 128))
        low = jnp.broadcast_to((label & 127).astype(BF16), (128, 128))
        col = slice(r * 128, (r + 1) * 128)
        within = jnp.broadcast_to((lane + (r % 2) * 128).astype(BF16), (tall16, 128))
        hit = high == high_of
        a_ref[0:tall16, col] = jnp.where(hit, jnp.bfloat16(r // 2), zero)
        a_ref[tall16:, col] = jnp.where(hit, within, zero)
        b_ref[:, col] = jnp.where(low == low_of, jnp.bfloat16(1), zero)
    found = lax.dot_general(a_ref[...], b_ref[...], (((1,), (1,)), ((), ())), preferred_element_type=F32)
    return found[0:tall16] * PAIR + found[tall16:]


def exchange_kernel(
    groups, places, edge, order_ref, node_ref, owned_ref, flag_ref, other_ref, raw_ref,
    grid_ref, delta_ref, change_ref,
    picked, inbox, reply, back, spot_ref, pa_ref, pb_ref, u_ref, tb_ref, sb_ref,
    send_out, recv_out, send_back, recv_back,
):
    fields, slots_all = change_ref.shape
    size = slots_all // (3 * places)
    heads = 2 * size // 128
    blocks = grid_ref.shape[1] // PAIR
    g, l = lax.axis_index("grp"), lax.axis_index("loc")

    far = [jnp.where(m > l, m - l, l - m) for m in range(places)]
    rank = [
        sum(((far[n] > far[m]) | ((far[n] == far[m]) & (n > m))).astype(I32) for n in range(places) if n != m)
        for m in range(places)
    ]
    places_by = [sum(jnp.where(rank[m] == i, m, 0) for m in range(places)) for i in range(places - 1)] + [l]

    def group(k):
        return lax.rem(g + groups + k, groups)

    def others(i):
        return (0, 2) if i == places - 1 else (0, 2, 1)

    def part(k, place):
        return pl.ds(pl.multiple_of((k * places + place) * size, 128), size)

    def lines_of(k, place):
        return [pl.ds((k * places + place) * (size // 128) + j, 1) for j in range(size // 128)]

    def copy(k, src, dst, there, near, sems, device):
        return pltpu.make_async_remote_copy(
            src_ref=src.at[:, part(k, there)],
            dst_ref=dst.at[:, part(k, near)],
            send_sem=sems[0].at[k * places + there],
            recv_sem=sems[1].at[k * places + near],
            device_id=device,
            device_id_type=MESH,
        )

    def outward(k, m):
        return copy(k, picked, inbox, m, l, (send_out, recv_out), (group(k - 1), m))

    def inward(k, m):
        return copy(k, picked, inbox, m, m, (send_out, recv_out), (group(1 - k), m))

    def homeward(k, m):
        return copy(k, reply, back, m, l, (send_back, recv_back), (group(1 - k), m))

    def returned(k, m):
        return copy(k, reply, back, m, m, (send_back, recv_back), (group(k - 1), m))

    barrier = pltpu.get_barrier_semaphore()
    for i in range(places):
        for k in others(i):
            pl.semaphore_signal(barrier, inc=1, device_id=(group(k - 1), places_by[i]), device_id_type=MESH)

    zero = jnp.bfloat16(0)
    where_is = find_nodes(edge, order_ref, pa_ref, pb_ref)
    grid_ref[...] = raw_ref[...]
    sweep(grid_ref, edge)
    for r in range(blocks):
        u_ref[r * 16 : (r + 1) * 16, :] = halves(grid_ref[:, r * PAIR : (r + 1) * PAIR])

    def spots_of(k, i):
        row = i * (spot_ref.shape[0] // places) + k * (size // 128)
        return jnp.concatenate([spot_ref[row + j : row + j + 1, :] for j in range(size // 128)], axis=1)

    def owned_of(k, m):
        return jnp.concatenate([owned_ref[line, :] for line in lines_of(k, m)], axis=1)

    def onehot(index, count):
        low = jnp.broadcast_to((index & (count - 1)).astype(BF16), (count, size))
        return jnp.where(low == iota((count, size), 0).astype(BF16), jnp.bfloat16(1), zero)

    tall = (((SIDE - 1) * edge + 1) ** 3 + 127) // 128

    def look_up(i, m):
        rows = [line for k in range(3) for line in lines_of(k, m)]
        spare = [jnp.full((8 - len(rows) % 8, 128), -1, I32)] if len(rows) % 8 else []
        node = jnp.concatenate([node_ref[line, :] for line in rows] + spare, axis=0)
        high, low = node >> 7, node & 127
        spot = jnp.full(node.shape, -float(PAIR), F32)
        for h in range(tall):
            row = jnp.broadcast_to(where_is[h : h + 1, :], node.shape)
            spot = jnp.where(high == h, jnp.take_along_axis(row, low, axis=1), spot)
        spot_ref[i * spot.shape[0] : (i + 1) * spot.shape[0], :] = spot.astype(I32)

    def pick_by_lane(spots):
        parts = []
        for j in range(size // 128):
            index = jnp.broadcast_to(spots[:, j * 128 : (j + 1) * 128], (fields, 128))
            which, low = index >> 7, index & 127
            value = jnp.zeros((fields, 128), F32)
            for r in range(2 * blocks):
                held = jnp.take_along_axis(grid_ref[:, r * 128 : (r + 1) * 128], low, axis=1)
                value = jnp.where(which == r, held, value)
            parts.append(value)
        return jnp.concatenate(parts, axis=1)

    general = jnp.concatenate([flag_ref[1:2, :]] * (size // 128), axis=1) > 0
    for i in range(places):
        m = places_by[i]
        look_up(i, m)
        by_lane = pick_by_lane(spots_of(1, i))
        picked[:, part(1, m)] = jnp.where(general, other_ref[:, part(1, m)], by_lane)
        for k in (0, 2):
            spots = spots_of(k, i)
            both = jnp.dot(u_ref[...], onehot(spots, PAIR), preferred_element_type=F32)
            which = jnp.broadcast_to(spots >> 8, (fields, size))
            top = jnp.zeros((fields, size), F32)
            rest = jnp.zeros((fields, size), F32)
            for r in range(blocks):
                mine = which == r
                top = jnp.where(mine, both[r * 16 : r * 16 + 8], top)
                rest = jnp.where(mine, both[r * 16 + 8 : r * 16 + 16], rest)
            picked[:, part(k, m)] = jnp.where(general, other_ref[:, part(k, m)], top + rest)
        if i == 1:
            pl.semaphore_wait(barrier, 3 * places - 1)
        for n in range(0 if i == 1 else i, i + 1 if i else 0):
            for k in others(n):
                outward(k, places_by[n]).start()

    for i in range(places):
        for k in range(3):
            column = ((places - 1 - i) * 3 + k) * size
            sb_ref[:, column : column + size] = onehot(spots_of(k, i), PAIR)
            tb_ref[:, part(k, places_by[i])] = onehot(owned_of(k, places_by[i]), 128)
    summed = jnp.zeros((heads * 16, 128), F32)
    for i in reversed(range(places)):
        m = places_by[i]
        for k in others(i):
            inward(k, m).wait_recv()
        lefts = []
        for k in range(3):
            source = picked if (i, k) == (places - 1, 1) else inbox
            both = halves(source[:, part(k, m)])
            which = jnp.broadcast_to((owned_of(k, m) >> 7).astype(BF16), (16, size))
            lefts.append(jnp.concatenate([jnp.where(which == jnp.bfloat16(h), both, zero) for h in range(heads)], axis=0))
        right = jnp.concatenate([tb_ref[:, part(k, m)] for k in range(3)], axis=1)
        summed = summed + lax.dot_general(
            jnp.concatenate(lefts, axis=1), right, (((1,), (1,)), ((), ())), preferred_element_type=F32
        )
    totals = [summed[h * 16 : h * 16 + 8] + summed[h * 16 + 8 : h * 16 + 16] for h in range(heads)]
    for i in range(places):
        m = places_by[i]
        for k in range(3):
            owned = owned_of(k, m)
            for j in range(size // 128):
                index = jnp.broadcast_to(owned[:, j * 128 : (j + 1) * 128], (fields, 128))
                low, which = index & 127, index >> 7
                total = jnp.zeros((fields, 128), F32)
                for h in range(heads):
                    total = jnp.where(which == h, jnp.take_along_axis(totals[h], low, axis=1), total)
                reply[:, pl.ds(pl.multiple_of((k * places + m) * size + j * 128, 128), 128)] = total
        for k in others(i):
            homeward(k, m).start()

    order = [i for i in reversed(range(places))]
    for first, last in tuple((n, n + 1) for n in range(places)):
        together = order[first:last]
        lefts = []
        for i in together:
            m = places_by[i]
            for k in others(i):
                returned(k, m).wait_recv()
            for k in range(3):
                source = reply if (i, k) == (places - 1, 1) else back
                change = source[:, part(k, m)] - picked[:, part(k, m)]
                change_ref[:, part(k, m)] = change
                both = halves(change)
                which = jnp.broadcast_to((spots_of(k, i) >> 8).astype(BF16), (16, size))
                lefts.append(jnp.concatenate([jnp.where(which == jnp.bfloat16(r), both, zero) for r in range(blocks)], axis=0))
        depth = len(together) * 3 * size
        start = first * 3 * size
        left = jnp.concatenate(lefts, axis=1)
        cut = blocks // 2 * 16
        spread = jnp.concatenate(
            [
                lax.dot_general(
                    part, sb_ref[:, start : start + depth], (((1,), (1,)), ((), ())), preferred_element_type=F32
                )
                for part in (left[:cut], left[cut:])
            ],
            axis=0,
        )
        for r in range(blocks):
            col = slice(r * PAIR, (r + 1) * PAIR)
            moved = spread[r * 16 : r * 16 + 8] + spread[r * 16 + 8 : r * 16 + 16]
            if first == 0:
                delta_ref[:, col] = moved
            else:
                delta_ref[:, col] += moved

    for i in range(places):
        for k in others(i):
            outward(k, places_by[i]).wait_send()
            homeward(k, places_by[i]).wait_send()


SMEM = pl.BlockSpec(memory_space=pltpu.SMEM)
VMEM = pl.BlockSpec(memory_space=pltpu.VMEM)
HBM = pl.BlockSpec(memory_space=pltpu.HBM)


def on_device(groups, places, element_values, local_map, send_node, send_count, recv_slot):
    fields, span = element_values.shape
    slots_all = send_node.shape[1]
    slot_count = slots_all // (3 * places)
    edge = blocks_along(span)
    local = ((SIDE - 1) * edge + 1) ** 3
    tall16 = (local + 2047) // 2048 * 16
    table = (local + 96) // 96 * 96
    lines, slot_rows = span // 128, slots_all // 128
    map_rows, node_rows = local_map.reshape(-1, 128), send_node.reshape(-1, 128)
    owned_rows = recv_slot.reshape(-1, 128)
    element_values, local_map, map_rows, node_rows, nodes, counts = (
        pltpu.with_memory_space_constraint(x, pltpu.HBM)
        for x in (element_values, local_map, map_rows, node_rows, send_node.reshape(-1), send_count.reshape(-1))
    )
    shape = jax.ShapeDtypeStruct
    general = [
        pltpu.SMEM((span,), I32),
        pltpu.SMEM((slots_all,), I32),
        pltpu.VMEM((span, 128), F32),
        pltpu.VMEM((table, 128), F32),
    ]
    order, live_nodes, flags, other, raw = pl.pallas_call(
        functools.partial(order_kernel, edge, slot_count),
        out_shape=(
            shape((lines, 128), I32),
            shape((slot_rows, 128), I32),
            shape((8, 128), I32),
            shape((fields, slots_all), F32),
            shape((fields, span), F32),
        ),
        in_specs=[HBM] * 6,
        out_specs=(VMEM,) * 5,
        scratch_shapes=[
            pltpu.VMEM((32 * ROWS, 128), I32),
            pltpu.VMEM((slot_rows, 128), I32),
            pltpu.SMEM(counts.shape, I32),
            pltpu.SemaphoreType.DMA((4,)),
            pltpu.VMEM((fields, span), F32),
        ]
        + general,
        compiler_params=pltpu.CompilerParams(vmem_limit_bytes=24 * 1024 * 1024),
    )(map_rows, node_rows, counts, element_values, local_map, nodes)
    grid, delta, change = pl.pallas_call(
        functools.partial(exchange_kernel, groups, places, edge),
        out_shape=(shape((fields, span), F32), shape((fields, span), F32), shape((fields, slots_all), F32)),
        in_specs=[VMEM] * 6,
        out_specs=(VMEM,) * 3,
        scratch_shapes=[pltpu.VMEM((fields, slots_all), F32)] * 4
        + [
            pltpu.VMEM((places * ((3 * slot_count // 128 + 7) // 8 * 8), 128), I32),
            pltpu.VMEM((2 * tall16, span), BF16),
            pltpu.VMEM((128, span), BF16),
            pltpu.VMEM((lines // 2 * 16, PAIR), BF16),
            pltpu.VMEM((128, slots_all), BF16),
            pltpu.VMEM((PAIR, slots_all), BF16),
        ]
        + [pltpu.SemaphoreType.DMA((3 * places,))] * 4,
        compiler_params=pltpu.CompilerParams(
            collective_id=0, has_side_effects=True, vmem_limit_bytes=40 * 1024 * 1024
        ),
    )(order, live_nodes, owned_rows, flags, other, raw)
    return pl.pallas_call(
        functools.partial(finish_kernel, edge, slot_count),
        out_shape=shape((fields, span), F32),
        in_specs=[VMEM] * 4 + [HBM] * 4,
        out_specs=HBM,
        scratch_shapes=[
            pltpu.VMEM((fields, span), F32),
            pltpu.SMEM((8, 128), I32),
            pltpu.SMEM(counts.shape, I32),
            pltpu.SemaphoreType.DMA((2,)),
        ]
        + general,
        compiler_params=pltpu.CompilerParams(vmem_limit_bytes=24 * 1024 * 1024),
    )(delta, grid, flags, change, counts, element_values, local_map, nodes)


def solution(mesh):
    return jax.shard_map(
        functools.partial(on_device, mesh.shape["grp"], mesh.shape["loc"]),
        mesh=mesh,
        in_specs=(
            P(None, ("grp", "loc")),
            P(("grp", "loc")),
            P(("grp", "loc"), None),
            P(("grp", "loc"), None),
            P(("grp", "loc"), None),
        ),
        out_specs=P(None, ("grp", "loc")),
        check_vma=False,
    )
```
